32 devices in a mesh: gx: 8 (over y, x, core), gy: 4 (over z).
Axes of the slice: x: 2, y: 2, z: 4, core: 2. Of those that a mesh axis runs over, the one named last changes fastest.
Arguments:
- fields: float32 [8, 2048, 2048], P(None, 'gx', 'gy'), may hold values from -6 to 6
- wave_order: int32 [1024], replicated, may hold values from 0 to 1023, as said below
- kept_mask: int32 [1024, 2048], P('gx', 'gy'), may hold values from 0 to 1, as said below
Outputs:
- spectral: float32 [2, 8, 1024, 2048], P(None, None, 'gx', 'gy')
The draws below stay inside these ranges and needn't reach their ends.
Inputs may be any that keep to these rules, and one draw needn't show every extreme that they name: `wave_order`: each x-wavenumber 0 to 1023 once. `kept_mask`: in each row the kept y-wavenumbers q are those with min(q, 2048 - q) up to a bound that does not grow with the row's x-wavenumber.
All inputs are finite; a program needn't handle non-finite values.
Results may differ from the reference program's by a relative error of at most 0.00007.
Values sent between devices are 32-bit elements; how exact they have to be, the bound alone decides.
No kernel may reach another device: no remote copies, remote signals or barrier semaphores. Data moves between devices by JAX's collectives and lax.ppermute only.
A program may use at most 192 MiB of HBM per device.

```python
import math
import jax
import jax.numpy as jnp

NX = 2048
NY = 2048
STACK = 8
KX = 1024


def common_draw(key):
    wave_order = jax.random.permutation(jax.random.fold_in(key, 11), KX).astype(jnp.int32)
    radius_x = jax.random.randint(jax.random.fold_in(key, 12), (), KX // 2, KX)
    radius_y = jax.random.randint(jax.random.fold_in(key, 13), (), NY // 4, NY // 2)
    y_waves = jnp.arange(NY, dtype=jnp.int32)
    folded = jnp.minimum(y_waves, NY - y_waves)
    scaled_x = wave_order * 1024 // radius_x
    scaled_y = folded * 1024 // radius_y
    inside = scaled_x[:, None] * scaled_x[:, None] + scaled_y[None, :] * scaled_y[None, :] <= 1024 * 1024
    return (wave_order, inside.astype(jnp.int32))


def draw_wave_order(key, part):
    return common_draw(key)[0]


def draw_kept_mask(key, part):
    return common_draw(key)[1]


def shard_levels(rng, dims, shards, low, top_value):
    gain = 1.0
    for axis_at, parts in shards:
        draws = jax.random.uniform(jax.random.fold_in(jax.random.fold_in(rng, 6), axis_at), (parts,), jnp.float32, low / len(shards), top_value / len(shards))
        gain = gain * jnp.repeat(jnp.exp(draws), dims[axis_at] // parts).reshape((-1,) + (1,) * (len(dims) - 1 - axis_at))
    return gain


def scatter_about(key, extent, scale, reach, split=(), kind=jnp.bfloat16):
    loudness = shard_levels(key, extent, split, -0.22, 0.18) if split else 1.0
    drawn = jax.random.normal(key, extent, jnp.float32) * scale * loudness
    return jnp.minimum(jnp.maximum(drawn, -reach), reach).astype(kind)


def setup_inputs(seed: int = 0) -> dict:
    key_of = jax.random.split(jax.random.key(seed), 4)
    fields = scatter_about(key_of[0], (STACK, NX, NY), 1.0, 6.0, ((1, 8), (2, 4)), jnp.float32)
    wave_order = draw_wave_order(jax.random.fold_in(key_of[3], 71), 0)
    kept_mask = draw_kept_mask(jax.random.fold_in(key_of[3], 71), 0)
    return {"fields": fields, "wave_order": wave_order, "kept_mask": kept_mask}


def reference(fields, wave_order, kept_mask):
    along_x = jnp.fft.fft(fields, axis=1)
    picked = jnp.take(along_x, wave_order, axis=1)
    both = jnp.fft.fft(picked, axis=2) / math.sqrt(NX * NY)
    weight = kept_mask.astype(jnp.float32)
    real_part = jnp.real(both).astype(jnp.float32) * weight
    imag_part = jnp.imag(both).astype(jnp.float32) * weight
    return jnp.stack([real_part, imag_part]).astype(jnp.float32)
```

```python
import math
from functools import partial

import jax
import jax.numpy as jnp
from jax import lax
from jax.experimental import pallas as pl
from jax.experimental.pallas import tpu as pltpu
from jax.sharding import PartitionSpec as P


X_RADIX = 8
Y_RADIX = 4
HALVES = 2
LANES = 128


def roots(numbers, period):
    angles = (numbers % period).astype(jnp.float32) * (2.0 * math.pi / period)
    return jnp.cos(angles), jnp.sin(angles)


def two_parts(values):
    high = lax.reduce_precision(values, 8, 7)
    return high.astype(jnp.bfloat16), (values - high).astype(jnp.bfloat16)


def x_table(period, kept, zero):
    points = jnp.arange(period // X_RADIX, dtype=jnp.int32) + zero
    units = jnp.arange(kept // X_RADIX, dtype=jnp.int32) * X_RADIX
    pairs = jnp.array([[0, 4], [1, 7], [2, 6], [3, 5]], dtype=jnp.int32)
    waves = pairs[:, :, None] + units[None, None, :]
    cos, sin = roots(waves[..., None] * points, period)
    table = jnp.stack([cos, sin], axis=2).reshape(4, 4 * units.shape[0], points.shape[0])
    return jnp.concatenate(two_parts(table), axis=2)


def y_table(period, scale, zero):
    short = period // Y_RADIX
    ids = jnp.arange(short, dtype=jnp.int32) + zero
    cos, sin = roots(ids[:, None] * ids[None, :], short)
    return jnp.stack(two_parts(jnp.concatenate([cos, sin], axis=1) * scale))


def y_twiddles(period, zero):
    ids = jnp.arange(period // Y_RADIX, dtype=jnp.int32) + zero
    cos, sin = roots(jnp.arange(Y_RADIX, dtype=jnp.int32)[:, None] * ids[None, :], period)
    return jnp.concatenate([cos, sin], axis=0)


def dot(left, right):
    return jnp.dot(left, right, preferred_element_type=jnp.float32)


def split(values):
    high = values.astype(jnp.bfloat16)
    return high, (values - high.astype(jnp.float32)).astype(jnp.bfloat16)


def pack_body(me_ref, *refs):
    count = len(refs) // 2
    for at in range(count):
        refs[count + at][...] = refs[at][0]


def pack(me, fields, first, columns):
    stack_count, rows, width = fields.shape
    lanes = width // columns
    gx = (stack_count // HALVES) * columns

    def spec(step):
        def index(_, me_ref):
            to = jnp.bitwise_xor(me_ref[0], step)
            return (first + to // columns, 0, to % columns)

        return pl.BlockSpec((1, rows, lanes), index)

    block = jax.ShapeDtypeStruct((rows, lanes), jnp.float32)
    return pl.pallas_call(
        pack_body,
        grid_spec=pltpu.PrefetchScalarGridSpec(
            num_scalar_prefetch=1,
            grid=(1,),
            in_specs=[spec(step) for step in range(1, gx)],
            out_specs=[pl.BlockSpec((rows, lanes), lambda *_: (0, 0)) for _ in range(1, gx)],
        ),
        out_shape=[block] * (gx - 1),
        name="pack",
    )(me, *([fields] * (gx - 1)))


def x_body(me_ref, where_ref, own_ref, *refs):
    others = refs[: X_RADIX - 1]
    table_ref, out_ref, line_ref, real_ref, imag_ref = refs[X_RADIX - 1 :]
    me = me_ref[0]
    line_ref[me] = own_ref[0]
    for step, ref in enumerate(others, 1):
        line_ref[jnp.bitwise_xor(me, step)] = ref[...]
    points, lanes = own_ref.shape[1:]
    units = real_ref.shape[0] // X_RADIX
    half = math.sqrt(0.5)
    f = [line_ref[at] for at in range(X_RADIX)]
    a = [f[at] + f[at + 4] for at in range(4)]
    d = [f[at] - f[at + 4] for at in range(4)]
    even, odd = a[0] + a[2], a[1] + a[3]
    less, more = (d[1] - d[3]) * half, (d[1] + d[3]) * half
    groups = (
        (0, 4, even + odd, even - odd),
        (1, 7, d[0] + less, -(d[2] + more)),
        (2, 6, a[0] - a[2], -(a[1] - a[3])),
        (3, 5, d[0] - less, d[2] - more),
    )
    for at, (c, e, left, right) in enumerate(groups):
        high, low = split(jnp.concatenate([left, right], axis=1))
        top = table_ref[at, :, :points]
        product = dot(top, high) + dot(table_ref[at, :, points:], high) + dot(top, low)
        cos_c, sin_c = product[:units], product[units : 2 * units]
        cos_e, sin_e = product[2 * units : 3 * units], product[3 * units :]
        rows_c, rows_e = pl.ds(c * units, units), pl.ds(e * units, units)
        if c == 0:
            real_ref[rows_c] = cos_c[:, :lanes]
            imag_ref[rows_c] = -sin_c[:, :lanes]
            real_ref[rows_e] = cos_e[:, lanes:]
            imag_ref[rows_e] = -sin_e[:, lanes:]
        else:
            real_ref[rows_c] = cos_c[:, :lanes] + sin_c[:, lanes:]
            imag_ref[rows_c] = cos_c[:, lanes:] - sin_c[:, :lanes]
            real_ref[rows_e] = cos_e[:, :lanes] - sin_e[:, lanes:]
            imag_ref[rows_e] = -cos_e[:, lanes:] - sin_e[:, :lanes]

    count, _, rows, _ = out_ref.shape

    def place(to, carry):
        for row in range(rows):
            source = where_ref[to * rows + row]
            out_ref[to, 0, pl.ds(row, 1), :] = real_ref[pl.ds(source, 1), :]
            out_ref[to, 1, pl.ds(row, 1), :] = imag_ref[pl.ds(source, 1), :]
        return carry

    lax.fori_loop(0, count, place, 0)


def x_lines(me, where, fields, first, columns, others, table, count):
    stack_count, rows, width = fields.shape
    lanes = width // columns
    kept = where.shape[0]

    def own(_, me_ref, where_ref):
        return (first + me_ref[0] // columns, 0, me_ref[0] % columns)

    whole = lambda *shape: pl.BlockSpec(shape, lambda *_: (0,) * len(shape))
    out = (count, 2, kept // count, lanes)
    return pl.pallas_call(
        x_body,
        grid_spec=pltpu.PrefetchScalarGridSpec(
            num_scalar_prefetch=2,
            grid=(1,),
            in_specs=[pl.BlockSpec((1, rows, lanes), own)]
            + [whole(rows, lanes)] * len(others)
            + [whole(*table.shape)],
            out_specs=whole(*out),
            scratch_shapes=[
                pltpu.VMEM((X_RADIX, rows, lanes), jnp.float32),
                pltpu.VMEM((kept, lanes), jnp.float32),
                pltpu.VMEM((kept, lanes), jnp.float32),
            ],
        ),
        out_shape=jax.ShapeDtypeStruct(out, jnp.float32),
        name="x_lines",
    )(me, where, fields, *others, table)


def y_body(me_ref, in_ref, twiddle_ref, table_ref, *refs):
    outs = refs[:Y_RADIX]
    high_ref, low_ref, wave_ref = refs[Y_RADIX:]
    me = me_ref[0]
    sources, _, rows, lanes = in_ref.shape
    short = table_ref.shape[1]
    columns = short // lanes
    levels = sources // (Y_RADIX * columns)
    block = levels * rows
    for level in range(levels):
        for column in range(columns):
            base = (level * columns + column) * Y_RADIX
            re = [in_ref[base + at, 0] for at in range(Y_RADIX)]
            im = [in_ref[base + at, 1] for at in range(Y_RADIX)]
            even_r, even_i, odd_r, odd_i = re[0] + re[2], im[0] + im[2], re[1] + re[3], im[1] + im[3]
            less_r, less_i, more_r, more_i = re[0] - re[2], im[0] - im[2], re[1] - re[3], im[1] - im[3]
            folded = (
                (even_r + odd_r, even_i + odd_i),
                (less_r + more_i, less_i - more_r),
                (even_r - odd_r, even_i - odd_i),
                (less_r - more_i, less_i + more_r),
            )
            span = pl.ds(column * lanes, lanes)
            for c, (real, imag) in enumerate(folded):
                if c:
                    cos = twiddle_ref[pl.ds(c, 1), span]
                    sin = twiddle_ref[pl.ds(Y_RADIX + c, 1), span]
                    real, imag = real * cos + imag * sin, imag * cos - real * sin
                for part, values in enumerate((real, imag)):
                    high, low = split(values)
                    at = pl.ds((c * 2 + part) * block + level * rows, rows)
                    high_ref[at, span] = high
                    low_ref[at, span] = low
    for c in range(Y_RADIX):
        at = pl.ds(c * 2 * block, 2 * block)
        product = dot(high_ref[at], table_ref[0]) + dot(low_ref[at], table_ref[0]) + dot(high_ref[at], table_ref[1])
        real = product[:block, :short] + product[block:, short:]
        imag = product[block:, :short] - product[:block, short:]
        for to in range(Y_RADIX):
            piece = slice(to * (short // Y_RADIX), (to + 1) * (short // Y_RADIX))
            wave_ref[c, to, :block] = real[:, piece]
            wave_ref[c, to, block:] = imag[:, piece]
    lane = lax.broadcasted_iota(jnp.int32, (rows, LANES), 1)
    residue = lane % Y_RADIX
    for step in range(Y_RADIX):
        to = jnp.bitwise_xor(me, step)
        for part in range(2):
            for level in range(levels):
                at = pl.ds(part * block + level * rows, rows)
                pieces = [wave_ref[c, to, at, :] for c in range(Y_RADIX)]
                for tile in range(Y_RADIX):
                    index = tile * (LANES // Y_RADIX) + lane // Y_RADIX
                    value = jnp.take_along_axis(pieces[0], index, axis=1, mode="promise_in_bounds")
                    for c in range(1, Y_RADIX):
                        other = jnp.take_along_axis(pieces[c], index, axis=1, mode="promise_in_bounds")
                        value = jnp.where(residue == c, other, value)
                    outs[step][part, level, :, pl.ds(tile * LANES, LANES)] = value


def y_lines(me, spectra, twiddles, table):
    sources, _, rows, lanes = spectra.shape
    short = table.shape[1]
    levels = sources * lanes // (Y_RADIX * short)
    whole = lambda *shape: pl.BlockSpec(shape, lambda *_: (0,) * len(shape))
    out = (2, levels, rows, short)
    tall = Y_RADIX * 2 * levels * rows
    return pl.pallas_call(
        y_body,
        grid_spec=pltpu.PrefetchScalarGridSpec(
            num_scalar_prefetch=1,
            grid=(1,),
            in_specs=[whole(*spectra.shape), whole(*twiddles.shape), whole(*table.shape)],
            out_specs=[whole(*out)] * Y_RADIX,
            scratch_shapes=[
                pltpu.VMEM((tall, short), jnp.bfloat16),
                pltpu.VMEM((tall, short), jnp.bfloat16),
                pltpu.VMEM((Y_RADIX, Y_RADIX, 2 * levels * rows, short // Y_RADIX), jnp.float32),
            ],
        ),
        out_shape=[jax.ShapeDtypeStruct(out, jnp.float32)] * Y_RADIX,
        name="y_lines",
    )(me, spectra, twiddles, table)


def finish_body(me_ref, *refs):
    blocks, mask_ref, out_ref = refs[:Y_RADIX], refs[Y_RADIX], refs[-1]
    rows = blocks[0].shape[2]
    for step, ref in enumerate(blocks):
        at = pl.ds(pl.multiple_of(jnp.bitwise_xor(me_ref[0], step) * rows, 8), rows)
        weight = mask_ref[at, :].astype(jnp.float32)
        for part in range(2):
            out_ref[part, 0, at, :] = ref[part, 0] * weight


def finish(me, blocks, kept_mask, first, stack_count, before):
    _, levels, rows, width = blocks[0].shape
    block = pl.BlockSpec((2, 1, rows, width), lambda level, me_ref: (0, level, 0, 0))
    extra = [] if before is None else [before]
    return pl.pallas_call(
        finish_body,
        grid_spec=pltpu.PrefetchScalarGridSpec(
            num_scalar_prefetch=1,
            grid=(levels,),
            in_specs=[block] * Y_RADIX
            + [pl.BlockSpec(kept_mask.shape, lambda level, me_ref: (0, 0))]
            + [pl.BlockSpec(memory_space=pl.ANY)] * len(extra),
            out_specs=pl.BlockSpec(
                (2, 1) + kept_mask.shape, lambda level, me_ref: (0, first + level, 0, 0)
            ),
        ),
        out_shape=jax.ShapeDtypeStruct((2, stack_count) + kept_mask.shape, jnp.float32),
        input_output_aliases={} if before is None else {2 + Y_RADIX: 0},
        name="finish",
    )(me, *blocks, kept_mask, *extra)


def exchange(blocks, axis, size):
    return [
        lax.ppermute(block, axis, [(at, at ^ step) for at in range(size)])
        for step, block in enumerate(blocks, 1)
    ]


def fast_shards(gx, gy, nx, ny, fields, wave_order, kept_mask):
    stack_count = fields.shape[0]
    kept = wave_order.shape[0]
    levels = stack_count // HALVES
    columns = gx // levels
    me_x, me_y = lax.axis_index("gx"), lax.axis_index("gy")
    zero = me_x // gx
    x_me, y_me = me_x.reshape(1).astype(jnp.int32), me_y.reshape(1).astype(jnp.int32)
    where = (wave_order % X_RADIX) * (kept // X_RADIX) + wave_order // X_RADIX
    firsts = [half * levels for half in range(HALVES)]
    lines = [exchange(pack(x_me, fields, first, columns), "gx", gx) for first in firsts]
    table_x = x_table(nx, kept, zero)
    table_y = y_table(ny, 1.0 / math.sqrt(nx * ny), zero)
    twiddles = y_twiddles(ny, zero)
    spectra = [
        lax.all_to_all(
            x_lines(x_me, where, fields, first, columns, line, table_x, gx * gy),
            ("gx", "gy"), split_axis=0, concat_axis=0, tiled=True,
        )
        for first, line in zip(firsts, lines)
    ]
    result = None
    waves = [y_lines(y_me, values, twiddles, table_y) for values in spectra]
    blocks = [[wave[0]] + exchange(wave[1:], "gy", gy) for wave in waves]
    for first, block in zip(firsts, blocks):
        result = finish(y_me, block, kept_mask, first, stack_count, result)
    return result


def wave_angles(wave_ids, points, period):
    phases = wave_ids[:, None] * points[None, :] % period
    angles = phases.astype(jnp.float32) * (2.0 * math.pi / period)
    return (jnp.cos(angles), jnp.sin(angles))


def x_terms(cos_table, sin_table, values):
    stack_count, x_count, y_count = values.shape
    waves = cos_table.shape[0]
    table = jnp.concatenate([cos_table, -sin_table], axis=0)
    flat = jnp.transpose(values, (1, 0, 2)).reshape(x_count, stack_count * y_count)
    product = jnp.dot(
        table, flat, precision=lax.Precision.HIGHEST, preferred_element_type=jnp.float32
    )
    product = product.reshape(2, waves, stack_count, y_count)
    return jnp.transpose(product, (1, 0, 2, 3))


def y_terms(cos_table, sin_table, spectra):
    rows, parts, stack_count, y_count = spectra.shape
    waves = cos_table.shape[0]
    table = jnp.concatenate([cos_table, sin_table], axis=0)
    flat = spectra.reshape(rows * parts * stack_count, y_count)
    product = jnp.dot(
        flat, table.T, precision=lax.Precision.HIGHEST, preferred_element_type=jnp.float32
    )
    product = product.reshape(rows, parts, stack_count, 2, waves)
    real_part = product[:, 0, :, 0] + product[:, 1, :, 1]
    imag_part = product[:, 1, :, 0] - product[:, 0, :, 1]
    return jnp.stack([real_part, imag_part], axis=1)


def plain_shards(nx, ny, fields, wave_order, kept_mask):
    x_every = jnp.arange(nx, dtype=jnp.int32)
    x_cos, x_sin = wave_angles(wave_order, x_every, nx)
    partial_terms = x_terms(
        x_cos, x_sin, lax.all_to_all(fields, "gx", split_axis=2, concat_axis=1, tiled=True)
    )
    spectra = lax.all_to_all(partial_terms, "gx", split_axis=0, concat_axis=3, tiled=True)
    y_every = jnp.arange(ny, dtype=jnp.int32)
    y_cos, y_sin = wave_angles(y_every, y_every, ny)
    y_spectra = y_terms(
        y_cos, y_sin, lax.all_to_all(spectra, "gy", split_axis=0, concat_axis=3, tiled=True)
    )
    result = lax.all_to_all(y_spectra, "gy", split_axis=3, concat_axis=0, tiled=True)
    weight = kept_mask.astype(jnp.float32) * (1.0 / math.sqrt(nx * ny))
    return jnp.transpose(result, (1, 2, 0, 3)) * weight[None, None]


def fits(gx, gy, stack_count, nx, ny, kept):
    levels = stack_count // HALVES
    if gx != X_RADIX or gy != Y_RADIX or stack_count % HALVES or gx % max(levels, 1):
        return False
    lanes = ny // gy // (gx // levels)
    return (
        lanes % LANES == 0
        and ny == Y_RADIX * Y_RADIX * LANES
        and nx % (X_RADIX * LANES) == 0
        and kept % (X_RADIX * LANES) == 0
        and kept <= nx
        and kept // (gx * gy) % 16 == 0
    )


def solution(mesh):
    gx, gy = mesh.shape["gx"], mesh.shape["gy"]

    def call(fields, wave_order, kept_mask):
        stack_count, nx, ny = fields.shape
        if fits(gx, gy, stack_count, nx, ny, wave_order.shape[0]):
            body = partial(fast_shards, gx, gy, nx, ny)
        else:
            body = partial(plain_shards, nx, ny)
        return jax.shard_map(
            body,
            mesh=mesh,
            in_specs=(P(None, "gx", "gy"), P(), P("gx", "gy")),
            out_specs=P(None, None, "gx", "gy"),
            check_vma=False,
        )(fields, wave_order, kept_mask)

    return call
```

```python
import math
from functools import partial

import jax
import jax.numpy as jnp
from jax import lax
from jax.experimental import pallas as pl
from jax.experimental.pallas import tpu as pltpu
from jax.sharding import PartitionSpec as P


X_RADIX = 8
Y_RADIX = 4
HALVES = 2
LANES = 128


def roots(numbers, period):
    angles = (numbers % period).astype(jnp.float32) * (2.0 * math.pi / period)
    return jnp.cos(angles), jnp.sin(angles)


def two_parts(values):
    high = lax.reduce_precision(values, 8, 7)
    return high.astype(jnp.bfloat16), (values - high).astype(jnp.bfloat16)


def x_table(period, kept, zero):
    points = jnp.arange(period // X_RADIX, dtype=jnp.int32) + zero
    units = jnp.arange(kept // X_RADIX, dtype=jnp.int32) * X_RADIX
    pairs = jnp.array([[0, 4], [1, 7], [2, 6], [3, 5]], dtype=jnp.int32)
    waves = pairs[:, :, None] + units[None, None, :]
    cos, sin = roots(waves[..., None] * points, period)
    table = jnp.stack([cos, sin], axis=2).reshape(4, 4 * units.shape[0], points.shape[0])
    return jnp.concatenate(two_parts(table), axis=2)


def y_table(period, scale, zero):
    short = period // Y_RADIX
    ids = jnp.arange(short, dtype=jnp.int32) + zero
    cos, sin = roots(ids[:, None] * ids[None, :], short)
    return jnp.stack(two_parts(jnp.concatenate([cos, sin], axis=1) * scale))


def y_twiddles(period, zero):
    ids = jnp.arange(period // Y_RADIX, dtype=jnp.int32) + zero
    cos, sin = roots(jnp.arange(Y_RADIX, dtype=jnp.int32)[:, None] * ids[None, :], period)
    return jnp.concatenate([cos, sin], axis=0)


def dot(left, right):
    return jnp.dot(left, right, preferred_element_type=jnp.float32)


def split(values):
    high = values.astype(jnp.bfloat16)
    return high, (values - high.astype(jnp.float32)).astype(jnp.bfloat16)


def pack_body(me_ref, *refs):
    count = len(refs) // 2
    for at in range(count):
        refs[count + at][...] = refs[at][0]


def pack(me, fields, first, columns):
    stack_count, rows, width = fields.shape
    lanes = width // columns
    gx = (stack_count // HALVES) * columns

    def spec(step):
        def index(_, me_ref):
            to = jnp.bitwise_xor(me_ref[0], step)
            return (first + to // columns, 0, to % columns)

        return pl.BlockSpec((1, rows, lanes), index)

    block = jax.ShapeDtypeStruct((rows, lanes), jnp.float32)
    return pl.pallas_call(
        pack_body,
        grid_spec=pltpu.PrefetchScalarGridSpec(
            num_scalar_prefetch=1,
            grid=(1,),
            in_specs=[spec(step) for step in range(1, gx)],
            out_specs=[pl.BlockSpec((rows, lanes), lambda *_: (0, 0)) for _ in range(1, gx)],
        ),
        out_shape=[block] * (gx - 1),
        name="pack",
    )(me, *([fields] * (gx - 1)))


def x_body(me_ref, where_ref, own_ref, *refs):
    others = refs[: X_RADIX - 1]
    table_ref, out_ref, line_ref, real_ref, imag_ref = refs[X_RADIX - 1 :]
    me = me_ref[0]
    line_ref[me] = own_ref[0]
    for step, ref in enumerate(others, 1):
        line_ref[jnp.bitwise_xor(me, step)] = ref[...]
    points, lanes = own_ref.shape[1:]
    units = real_ref.shape[0] // X_RADIX
    half = math.sqrt(0.5)
    f = [line_ref[at] for at in range(X_RADIX)]
    a = [f[at] + f[at + 4] for at in range(4)]
    d = [f[at] - f[at + 4] for at in range(4)]
    even, odd = a[0] + a[2], a[1] + a[3]
    less, more = (d[1] - d[3]) * half, (d[1] + d[3]) * half
    groups = (
        (0, 4, even + odd, even - odd),
        (1, 7, d[0] + less, -(d[2] + more)),
        (2, 6, a[0] - a[2], -(a[1] - a[3])),
        (3, 5, d[0] - less, d[2] - more),
    )
    for at, (c, e, left, right) in enumerate(groups):
        high, low = split(jnp.concatenate([left, right], axis=1))
        top = table_ref[at, :, :points]
        product = dot(top, high) + dot(table_ref[at, :, points:], high) + dot(top, low)
        cos_c, sin_c = product[:units], product[units : 2 * units]
        cos_e, sin_e = product[2 * units : 3 * units], product[3 * units :]
        rows_c, rows_e = pl.ds(c * units, units), pl.ds(e * units, units)
        if c == 0:
            real_ref[rows_c] = cos_c[:, :lanes]
            imag_ref[rows_c] = -sin_c[:, :lanes]
            real_ref[rows_e] = cos_e[:, lanes:]
            imag_ref[rows_e] = -sin_e[:, lanes:]
        else:
            real_ref[rows_c] = cos_c[:, :lanes] + sin_c[:, lanes:]
            imag_ref[rows_c] = cos_c[:, lanes:] - sin_c[:, :lanes]
            real_ref[rows_e] = cos_e[:, :lanes] - sin_e[:, lanes:]
            imag_ref[rows_e] = -cos_e[:, lanes:] - sin_e[:, :lanes]

    count, _, rows, _ = out_ref.shape

    def place(to, carry):
        for row in range(rows):
            source = where_ref[to * rows + row]
            out_ref[to, 0, pl.ds(row, 1), :] = real_ref[pl.ds(source, 1), :]
            out_ref[to, 1, pl.ds(row, 1), :] = imag_ref[pl.ds(source, 1), :]
        return carry

    lax.fori_loop(0, count, place, 0)


def x_lines(me, where, fields, first, columns, others, table, count):
    _, rows, width = fields.shape
    lanes = width // columns
    kept = where.shape[0]

    def own(_, me_ref, where_ref):
        return (first + me_ref[0] // columns, 0, me_ref[0] % columns)

    whole = lambda *shape: pl.BlockSpec(shape, lambda *_: (0,) * len(shape))
    out = (count, 2, kept // count, lanes)
    return pl.pallas_call(
        x_body,
        grid_spec=pltpu.PrefetchScalarGridSpec(
            num_scalar_prefetch=2,
            grid=(1,),
            in_specs=[pl.BlockSpec((1, rows, lanes), own)]
            + [whole(rows, lanes)] * len(others)
            + [whole(*table.shape)],
            out_specs=whole(*out),
            scratch_shapes=[
                pltpu.VMEM((X_RADIX, rows, lanes), jnp.float32),
                pltpu.VMEM((kept, lanes), jnp.float32),
                pltpu.VMEM((kept, lanes), jnp.float32),
            ],
        ),
        out_shape=jax.ShapeDtypeStruct(out, jnp.float32),
        name="x_lines",
    )(me, where, fields, *others, table)


def y_body(me_ref, in_ref, twiddle_ref, table_ref, *refs):
    outs = refs[:Y_RADIX]
    high_ref, low_ref, wave_ref = refs[Y_RADIX:]
    me = me_ref[0]
    sources, _, rows, lanes = in_ref.shape
    short = table_ref.shape[1]
    columns = short // lanes
    levels = sources // (Y_RADIX * columns)
    block = levels * rows
    for level in range(levels):
        for column in range(columns):
            base = (level * columns + column) * Y_RADIX
            re = [in_ref[base + at, 0] for at in range(Y_RADIX)]
            im = [in_ref[base + at, 1] for at in range(Y_RADIX)]
            even_r, even_i, odd_r, odd_i = re[0] + re[2], im[0] + im[2], re[1] + re[3], im[1] + im[3]
            less_r, less_i, more_r, more_i = re[0] - re[2], im[0] - im[2], re[1] - re[3], im[1] - im[3]
            folded = (
                (even_r + odd_r, even_i + odd_i),
                (less_r + more_i, less_i - more_r),
                (even_r - odd_r, even_i - odd_i),
                (less_r - more_i, less_i + more_r),
            )
            span = pl.ds(column * lanes, lanes)
            for c, (real, imag) in enumerate(folded):
                if c:
                    cos = twiddle_ref[pl.ds(c, 1), span]
                    sin = twiddle_ref[pl.ds(Y_RADIX + c, 1), span]
                    real, imag = real * cos + imag * sin, imag * cos - real * sin
                for part, values in enumerate((real, imag)):
                    high, low = split(values)
                    at = pl.ds((c * 2 + part) * block + level * rows, rows)
                    high_ref[at, span] = high
                    low_ref[at, span] = low
    for c in range(Y_RADIX):
        at = pl.ds(c * 2 * block, 2 * block)
        product = dot(high_ref[at], table_ref[0]) + dot(low_ref[at], table_ref[0]) + dot(high_ref[at], table_ref[1])
        real = product[:block, :short] + product[block:, short:]
        imag = product[block:, :short] - product[:block, short:]
        for to in range(Y_RADIX):
            piece = slice(to * (short // Y_RADIX), (to + 1) * (short // Y_RADIX))
            wave_ref[c, to, :block] = real[:, piece]
            wave_ref[c, to, block:] = imag[:, piece]
    lane = lax.broadcasted_iota(jnp.int32, (rows, LANES), 1)
    residue = lane % Y_RADIX
    for step in range(Y_RADIX):
        to = jnp.bitwise_xor(me, step)
        for part in range(2):
            for level in range(levels):
                at = pl.ds(part * block + level * rows, rows)
                pieces = [wave_ref[c, to, at, :] for c in range(Y_RADIX)]
                for tile in range(Y_RADIX):
                    index = tile * (LANES // Y_RADIX) + lane // Y_RADIX
                    value = jnp.take_along_axis(pieces[0], index, axis=1, mode="promise_in_bounds")
                    for c in range(1, Y_RADIX):
                        other = jnp.take_along_axis(pieces[c], index, axis=1, mode="promise_in_bounds")
                        value = jnp.where(residue == c, other, value)
                    outs[step][part, level, :, pl.ds(tile * LANES, LANES)] = value


def y_lines(me, spectra, twiddles, table):
    sources, _, rows, lanes = spectra.shape
    short = table.shape[1]
    levels = sources * lanes // (Y_RADIX * short)
    whole = lambda *shape: pl.BlockSpec(shape, lambda *_: (0,) * len(shape))
    out = (2, levels, rows, short)
    tall = Y_RADIX * 2 * levels * rows
    return pl.pallas_call(
        y_body,
        grid_spec=pltpu.PrefetchScalarGridSpec(
            num_scalar_prefetch=1,
            grid=(1,),
            in_specs=[whole(*spectra.shape), whole(*twiddles.shape), whole(*table.shape)],
            out_specs=[whole(*out)] * Y_RADIX,
            scratch_shapes=[
                pltpu.VMEM((tall, short), jnp.bfloat16),
                pltpu.VMEM((tall, short), jnp.bfloat16),
                pltpu.VMEM((Y_RADIX, Y_RADIX, 2 * levels * rows, short // Y_RADIX), jnp.float32),
            ],
        ),
        out_shape=[jax.ShapeDtypeStruct(out, jnp.float32)] * Y_RADIX,
        name="y_lines",
    )(me, spectra, twiddles, table)


def finish_body(me_ref, *refs):
    blocks, mask_ref, out_ref = refs[:Y_RADIX], refs[Y_RADIX], refs[-1]
    rows = blocks[0].shape[2]
    for step, ref in enumerate(blocks):
        at = pl.ds(pl.multiple_of(jnp.bitwise_xor(me_ref[0], step) * rows, 8), rows)
        weight = mask_ref[at, :].astype(jnp.float32)
        for part in range(2):
            out_ref[part, 0, at, :] = ref[part, 0] * weight


def finish(me, blocks, kept_mask, first, stack_count, before):
    _, levels, rows, width = blocks[0].shape
    block = pl.BlockSpec((2, 1, rows, width), lambda level, me_ref: (0, level, 0, 0))
    extra = [] if before is None else [before]
    return pl.pallas_call(
        finish_body,
        grid_spec=pltpu.PrefetchScalarGridSpec(
            num_scalar_prefetch=1,
            grid=(levels,),
            in_specs=[block] * Y_RADIX
            + [pl.BlockSpec(kept_mask.shape, lambda level, me_ref: (0, 0))]
            + [pl.BlockSpec(memory_space=pl.ANY)] * len(extra),
            out_specs=pl.BlockSpec(
                (2, 1) + kept_mask.shape, lambda level, me_ref: (0, first + level, 0, 0)
            ),
        ),
        out_shape=jax.ShapeDtypeStruct((2, stack_count) + kept_mask.shape, jnp.float32),
        input_output_aliases={} if before is None else {2 + Y_RADIX: 0},
        name="finish",
    )(me, *blocks, kept_mask, *extra)


def turn(values):
    lane = lax.broadcasted_iota(jnp.int32, values.shape, 1)
    rolled = pltpu.roll(values, LANES // 2, 1)
    return jnp.where(lane < LANES // 2, rolled, -rolled)


def y_first_body(scale, me_ref, own_ref, *refs):
    others = refs[: Y_RADIX - 1]
    twiddle_ref, table_ref = refs[Y_RADIX - 1 : Y_RADIX + 1]
    outs = refs[Y_RADIX + 1 : Y_RADIX + 1 + X_RADIX]
    field_ref, wave_ref = refs[Y_RADIX + 1 + X_RADIX :]
    me_x, me_y = me_ref[0], me_ref[1]
    rows, short = own_ref.shape[1:]
    half = short // 2
    field_ref[me_y] = own_ref[0]
    for step, ref in enumerate(others, 1):
        field_ref[jnp.bitwise_xor(me_y, step)] = ref[...]
    even, odd = field_ref[0] + field_ref[2], field_ref[1] + field_ref[3]
    less, more = field_ref[0] - field_ref[2], field_ref[1] - field_ref[3]
    folded = ((even + odd, None), (less, -more), (even - odd, None), (less, more))
    for c, (real, imag) in enumerate(folded):
        if c:
            cos, sin = twiddle_ref[pl.ds(c, 1), :], twiddle_ref[pl.ds(Y_RADIX + c, 1), :]
            if imag is None:
                real, imag = real * cos, -real * sin
            else:
                real, imag = real * cos + imag * sin, imag * cos - real * sin
        tall = real if imag is None else jnp.concatenate([real, imag], axis=0)
        high, low = split(tall)
        parts = []
        for span in (pl.ds(0, half), pl.ds(short, half)):
            parts.append(dot(high, table_ref[0, :, span]) + dot(low, table_ref[0, :, span]) + dot(high, table_ref[1, :, span]))
        by_cos, by_sin = parts
        if imag is None:
            point = lax.broadcasted_iota(jnp.int32, real.shape, 1)
            top = jnp.sum(jnp.where(point % 2 == 0, real, -real), axis=1, keepdims=True) * scale
            unit = lax.broadcasted_iota(jnp.int32, by_sin.shape, 1)
            wave_ref[c, 0] = by_cos
            wave_ref[c, 1] = jnp.where(unit == 0, top, -by_sin)
        else:
            wave_ref[c, 0] = by_cos[:rows] + by_sin[rows:]
            wave_ref[c, 1] = by_cos[rows:] - by_sin[:rows]
    chunk = 32

    def place(at, carry):
        span = pl.ds(pl.multiple_of(at * chunk, chunk), chunk)
        lane = lax.broadcasted_iota(jnp.int32, (chunk, LANES), 1)
        local = lane % (LANES // 2)
        for step in range(X_RADIX):
            to = jnp.bitwise_xor(me_x, step)
            index = to * (LANES // 2 // Y_RADIX) + local // Y_RADIX
            for side in range(2):
                units = pl.ds(side * LANES, LANES)
                value = None
                for c in range(Y_RADIX):
                    pair = [
                        jnp.take_along_axis(wave_ref[c, part, span, units], index, axis=1, mode="promise_in_bounds")
                        for part in range(2)
                    ]
                    both = jnp.where(lane < LANES // 2, *pair)
                    value = both if c == 0 else jnp.where(lane % Y_RADIX == c, both, value)
                outs[step][span, units] = value
        return carry

    lax.fori_loop(0, rows // chunk, place, 0)


def y_first(me, scale, fields, first, others, twiddles, table):
    _, rows, short = fields.shape
    whole = lambda *shape: pl.BlockSpec(shape, lambda *_: (0,) * len(shape))
    out = (rows, 2 * LANES)
    return pl.pallas_call(
        partial(y_first_body, scale),
        grid_spec=pltpu.PrefetchScalarGridSpec(
            num_scalar_prefetch=1,
            grid=(1,),
            in_specs=[pl.BlockSpec((1, rows, short), lambda _, me_ref: (first + me_ref[1], 0, 0))]
            + [whole(rows, short)] * len(others)
            + [whole(*twiddles.shape), whole(*table.shape)],
            out_specs=[whole(*out)] * X_RADIX,
            scratch_shapes=[
                pltpu.VMEM((Y_RADIX, rows, short), jnp.float32),
                pltpu.VMEM((Y_RADIX, 2, rows, short // 2), jnp.float32),
            ],
        ),
        out_shape=[jax.ShapeDtypeStruct(out, jnp.float32)] * X_RADIX,
        name="y_first",
    )(me, fields, *others, twiddles, table)


def x_second_body(me_ref, where_ref, *refs):
    blocks = refs[:X_RADIX]
    table_ref, out_ref, fold_ref, wave_ref = refs[X_RADIX:]
    me = me_ref[0]
    points = blocks[0].shape[0]
    units = wave_ref.shape[1] // X_RADIX
    for step, ref in enumerate(blocks):
        fold_ref[jnp.bitwise_xor(me, step)] = ref[...]
    half = math.sqrt(0.5)
    for side in range(2):
        span = pl.ds(side * LANES, LANES)
        f = [fold_ref[at, :, span] for at in range(X_RADIX)]
        a = [f[at] + f[at + 4] for at in range(4)]
        d = [f[at] - f[at + 4] for at in range(4)]
        even, odd, less, more = a[0] + a[2], a[1] + a[3], a[0] - a[2], turn(a[1] - a[3])
        across, along = turn(d[2]), turn(d[1] + d[3])
        one = (d[1] - d[3] + along) * half
        three = (along - d[1] + d[3]) * half
        folded = {
            0: even + odd,
            4: even - odd,
            2: less + more,
            6: less - more,
            1: d[0] + across + one,
            5: d[0] + across - one,
            3: d[0] - across + three,
            7: d[0] - across - three,
        }
        for c, values in folded.items():
            fold_ref[c, :, span] = values
    lane = lax.broadcasted_iota(jnp.int32, (points, 2 * LANES), 1)
    sign = jnp.where(lane % LANES < LANES // 2, 1.0, -1.0)
    lane = lax.broadcasted_iota(jnp.int32, (units, LANES), 1)
    special = jnp.logical_and(lane % (LANES // 2) == 0, me == 0)
    for at, pair in enumerate(((0, 4), (1, 7), (2, 6), (3, 5))):
        for side, c in enumerate(pair):
            data = jnp.concatenate([fold_ref[c], fold_ref[-c % X_RADIX] * sign], axis=1)
            high, low = split(data)
            rows = pl.ds(side * 2 * units, 2 * units)
            top = table_ref[at, rows, :points]
            product = dot(top, high) + dot(table_ref[at, rows, points:], high) + dot(top, low)
            plus_low, plus_high, minus_low, minus_high = (
                product[:units, piece * LANES : (piece + 1) * LANES]
                + turn(product[units:, piece * LANES : (piece + 1) * LANES])
                for piece in range(4)
            )
            rows = pl.ds(c * units, units)
            wave_ref[0, rows] = jnp.where(special, (plus_low + minus_low) * 0.5, plus_low)
            wave_ref[1, rows] = plus_high
            wave_ref[2, rows] = jnp.where(special, turn(plus_low - minus_low) * 0.5, minus_high)
            wave_ref[3, rows] = jnp.where(special, minus_high, minus_low)

    count, rows, _ = out_ref.shape
    unroll = 32

    def place(at, carry):
        to, start = at // (rows // unroll) * Y_RADIX, at % (rows // unroll) * unroll
        for row in range(unroll):
            source = where_ref[at * unroll + row]
            for piece in range(Y_RADIX):
                out_ref[to + piece, pl.ds(start + row, 1), :] = wave_ref[piece, pl.ds(source, 1), :]
        return carry

    lax.fori_loop(0, count // Y_RADIX * (rows // unroll), place, 0)


def x_second(me, where, blocks, table, gx):
    points, lanes = blocks[0].shape
    kept = where.shape[0]
    whole = lambda *shape: pl.BlockSpec(shape, lambda *_: (0,) * len(shape))
    out = (gx * Y_RADIX, kept // gx, LANES)
    return pl.pallas_call(
        x_second_body,
        grid_spec=pltpu.PrefetchScalarGridSpec(
            num_scalar_prefetch=2,
            grid=(1,),
            in_specs=[whole(points, lanes)] * X_RADIX + [whole(*table.shape)],
            out_specs=whole(*out),
            scratch_shapes=[
                pltpu.VMEM((X_RADIX, points, lanes), jnp.float32),
                pltpu.VMEM((Y_RADIX, kept, LANES), jnp.float32),
            ],
        ),
        out_shape=jax.ShapeDtypeStruct(out, jnp.float32),
        name="x_second",
    )(me, where, *blocks, table)


def finish_second_body(me_ref, in_ref, mask_ref, before_ref, out_ref):
    mirrored = me_ref[0] >= Y_RADIX // 2
    rows = mask_ref.shape[0]
    chunk = 32

    def place(at, carry):
        span = pl.ds(pl.multiple_of(at * chunk, chunk), chunk)
        lane = lax.broadcasted_iota(jnp.int32, (chunk, LANES), 1)
        left = lane < LANES // 2
        index = jnp.where(mirrored, (LANES - lane) % LANES, lane)
        for tile in range(Y_RADIX):
            body = jnp.where(mirrored, Y_RADIX - 1 - tile, tile)
            head = jnp.where(mirrored, (Y_RADIX - tile) % Y_RADIX, tile)
            here, there = in_ref[2 * body, 0, span, :], in_ref[2 * body + 1, 0, span, :]
            start = in_ref[2 * head, 0, span, :]
            real = jnp.where(left, here, pltpu.roll(there, LANES // 2, 1))
            imag = jnp.where(left, pltpu.roll(here, LANES // 2, 1), there)
            lanes = pl.ds(tile * LANES, LANES)
            weight = mask_ref[span, lanes].astype(jnp.float32)
            for part, (values, edge) in enumerate(((real, start), (imag, pltpu.roll(start, LANES // 2, 1)))):
                values = jnp.take_along_axis(values, index, axis=1, mode="promise_in_bounds")
                out_ref[part, 0, span, lanes] = jnp.where(lane == 0, edge, values) * weight
        return carry

    lax.fori_loop(0, rows // chunk, place, 0)


def finish_second(me, blocks, kept_mask, first, before):
    gx, levels, rows, lanes = blocks.shape
    return pl.pallas_call(
        finish_second_body,
        grid_spec=pltpu.PrefetchScalarGridSpec(
            num_scalar_prefetch=1,
            grid=(levels,),
            in_specs=[
                pl.BlockSpec((gx, 1, rows, lanes), lambda level, me_ref: (0, level, 0, 0)),
                pl.BlockSpec(kept_mask.shape, lambda level, me_ref: (0, 0)),
                pl.BlockSpec(memory_space=pl.ANY),
            ],
            out_specs=pl.BlockSpec(
                (2, 1) + kept_mask.shape, lambda level, me_ref: (0, first + level, 0, 0)
            ),
        ),
        out_shape=jax.ShapeDtypeStruct(before.shape, jnp.float32),
        input_output_aliases={3: 0},
        name="finish_second",
    )(me, blocks, kept_mask, before)


def exchange(blocks, axis, size):
    return [
        lax.ppermute(block, axis, [(at, at ^ step) for at in range(size)])
        for step, block in enumerate(blocks, 1)
    ]


def fast_shards(gx, gy, nx, ny, fields, wave_order, kept_mask):
    stack_count = fields.shape[0]
    kept = wave_order.shape[0]
    levels = stack_count // HALVES
    columns = gx // levels
    me_x, me_y = lax.axis_index("gx"), lax.axis_index("gy")
    zero = me_x // gx
    x_me, y_me = me_x.reshape(1).astype(jnp.int32), me_y.reshape(1).astype(jnp.int32)
    where = (wave_order % X_RADIX) * (kept // X_RADIX) + wave_order // X_RADIX
    both_me = jnp.concatenate([x_me, y_me])
    scale = 1.0 / math.sqrt(nx * ny)
    whole = ("gx", "gy")
    second = levels
    fields_second = exchange(pack(y_me, fields, second, 1), "gy", gy)
    lines = exchange(pack(x_me, fields, 0, columns), "gx", gx)
    table_x = x_table(nx, kept, zero)
    table_y = y_table(ny, scale, zero)
    twiddles = y_twiddles(ny, zero)
    spectra = x_lines(x_me, where, fields, 0, columns, lines, table_x, gx * gy)
    spectra = lax.all_to_all(spectra, whole, split_axis=0, concat_axis=0, tiled=True)
    half_waves = y_first(both_me, scale, fields, second, fields_second, twiddles, table_y)
    half_waves = [half_waves[0]] + exchange(half_waves[1:], "gx", gx)
    waves = y_lines(y_me, spectra, twiddles, table_y)
    waves = [waves[0]] + exchange(waves[1:], "gy", gy)
    owned = x_second(x_me, where, half_waves, table_x, gx)
    owned = lax.all_to_all(owned, whole, split_axis=0, concat_axis=0, tiled=True)
    result = finish(y_me, waves, kept_mask, 0, stack_count, None)
    owned = owned.reshape((gx, gy) + owned.shape[1:])
    return finish_second(y_me, owned, kept_mask, second, result)


def wave_angles(wave_ids, points, period):
    phases = wave_ids[:, None] * points[None, :] % period
    angles = phases.astype(jnp.float32) * (2.0 * math.pi / period)
    return (jnp.cos(angles), jnp.sin(angles))


def x_terms(cos_table, sin_table, values):
    stack_count, x_count, y_count = values.shape
    waves = cos_table.shape[0]
    table = jnp.concatenate([cos_table, -sin_table], axis=0)
    flat = jnp.transpose(values, (1, 0, 2)).reshape(x_count, stack_count * y_count)
    product = jnp.dot(
        table, flat, precision=lax.Precision.HIGHEST, preferred_element_type=jnp.float32
    )
    product = product.reshape(2, waves, stack_count, y_count)
    return jnp.transpose(product, (1, 0, 2, 3))


def y_terms(cos_table, sin_table, spectra):
    rows, parts, stack_count, y_count = spectra.shape
    waves = cos_table.shape[0]
    table = jnp.concatenate([cos_table, sin_table], axis=0)
    flat = spectra.reshape(rows * parts * stack_count, y_count)
    product = jnp.dot(
        flat, table.T, precision=lax.Precision.HIGHEST, preferred_element_type=jnp.float32
    )
    product = product.reshape(rows, parts, stack_count, 2, waves)
    real_part = product[:, 0, :, 0] + product[:, 1, :, 1]
    imag_part = product[:, 1, :, 0] - product[:, 0, :, 1]
    return jnp.stack([real_part, imag_part], axis=1)


def plain_shards(nx, ny, fields, wave_order, kept_mask):
    x_every = jnp.arange(nx, dtype=jnp.int32)
    x_cos, x_sin = wave_angles(wave_order, x_every, nx)
    partial_terms = x_terms(
        x_cos, x_sin, lax.all_to_all(fields, "gx", split_axis=2, concat_axis=1, tiled=True)
    )
    spectra = lax.all_to_all(partial_terms, "gx", split_axis=0, concat_axis=3, tiled=True)
    y_every = jnp.arange(ny, dtype=jnp.int32)
    y_cos, y_sin = wave_angles(y_every, y_every, ny)
    y_spectra = y_terms(
        y_cos, y_sin, lax.all_to_all(spectra, "gy", split_axis=0, concat_axis=3, tiled=True)
    )
    result = lax.all_to_all(y_spectra, "gy", split_axis=3, concat_axis=0, tiled=True)
    weight = kept_mask.astype(jnp.float32) * (1.0 / math.sqrt(nx * ny))
    return jnp.transpose(result, (1, 2, 0, 3)) * weight[None, None]


def fits(gx, gy, stack_count, nx, ny, kept):
    levels = stack_count // HALVES
    if gx != X_RADIX or gy != Y_RADIX or levels != gy or stack_count % HALVES:
        return False
    lanes = ny // gy // (gx // levels)
    return (
        lanes % LANES == 0
        and ny == Y_RADIX * Y_RADIX * LANES
        and nx % (X_RADIX * LANES) == 0
        and kept % (X_RADIX * LANES) == 0
        and kept <= nx
        and kept // (gx * gy) % 16 == 0
    )


def solution(mesh):
    gx, gy = mesh.shape["gx"], mesh.shape["gy"]

    def call(fields, wave_order, kept_mask):
        stack_count, nx, ny = fields.shape
        if fits(gx, gy, stack_count, nx, ny, wave_order.shape[0]):
            body = partial(fast_shards, gx, gy, nx, ny)
        else:
            body = partial(plain_shards, nx, ny)
        return jax.shard_map(
            body,
            mesh=mesh,
            in_specs=(P(None, "gx", "gy"), P(), P("gx", "gy")),
            out_specs=P(None, None, "gx", "gy"),
            check_vma=False,
        )(fields, wave_order, kept_mask)

    return call
```

```python
import math
from functools import partial

import jax
import jax.numpy as jnp
from jax import lax
from jax.experimental import pallas as pl
from jax.experimental.pallas import tpu as pltpu
from jax.sharding import PartitionSpec as P


X_RADIX = 8
Y_RADIX = 4
HALVES = 2
PIECES = 2
LANES = 128


def roots(numbers, period):
    angles = (numbers % period).astype(jnp.float32) * (2.0 * math.pi / period)
    return jnp.cos(angles), jnp.sin(angles)


def two_parts(values):
    high = lax.reduce_precision(values, 8, 7)
    return high.astype(jnp.bfloat16), (values - high).astype(jnp.bfloat16)


def x_table(period, kept, zero):
    points = jnp.arange(period // X_RADIX, dtype=jnp.int32) + zero
    units = jnp.arange(kept // X_RADIX, dtype=jnp.int32) * X_RADIX
    pairs = jnp.array([[0, 4], [1, 7], [2, 6], [3, 5]], dtype=jnp.int32)
    waves = pairs[:, :, None] + units[None, None, :]
    cos, sin = roots(waves[..., None] * points, period)
    table = jnp.stack([cos, sin], axis=2).reshape(4, 4 * units.shape[0], points.shape[0])
    return jnp.concatenate(two_parts(table), axis=2)


def y_table(period, scale, zero):
    short = period // Y_RADIX
    ids = jnp.arange(short, dtype=jnp.int32) + zero
    cos, sin = roots(ids[:, None] * ids[None, :], short)
    return jnp.stack(two_parts(jnp.concatenate([cos, sin], axis=1) * scale))


def y_twiddles(period, zero):
    ids = jnp.arange(period // Y_RADIX, dtype=jnp.int32) + zero
    cos, sin = roots(jnp.arange(Y_RADIX, dtype=jnp.int32)[:, None] * ids[None, :], period)
    return jnp.concatenate([cos, sin], axis=0)


def dot(left, right):
    return jnp.dot(left, right, preferred_element_type=jnp.float32)


def split(values):
    high = values.astype(jnp.bfloat16)
    return high, (values - high.astype(jnp.float32)).astype(jnp.bfloat16)


def pack_body(me_ref, *refs):
    count = len(refs) // 2
    for at in range(count):
        refs[count + at][...] = refs[at][0]


def pack(me, fields, first, columns):
    stack_count, rows, width = fields.shape
    lanes = width // columns
    gx = (stack_count // HALVES) * columns

    def spec(step):
        def index(_, me_ref):
            to = jnp.bitwise_xor(me_ref[0], step)
            return (first + to // columns, 0, to % columns)

        return pl.BlockSpec((1, rows, lanes), index)

    block = jax.ShapeDtypeStruct((rows, lanes), jnp.float32)
    return pl.pallas_call(
        pack_body,
        grid_spec=pltpu.PrefetchScalarGridSpec(
            num_scalar_prefetch=1,
            grid=(1,),
            in_specs=[spec(step) for step in range(1, gx)],
            out_specs=[pl.BlockSpec((rows, lanes), lambda *_: (0, 0)) for _ in range(1, gx)],
        ),
        out_shape=[block] * (gx - 1),
        name="pack",
    )(me, *([fields] * (gx - 1)))


def x_body(gy, me_ref, where_ref, own_ref, *refs):
    others = refs[: X_RADIX - 1]
    table_ref, line_ref, real_ref, imag_ref = refs[X_RADIX - 1], *refs[X_RADIX + PIECES :]
    outs = refs[X_RADIX : X_RADIX + PIECES]
    me = me_ref[0]
    line_ref[me] = own_ref[0]
    for step, ref in enumerate(others, 1):
        line_ref[jnp.bitwise_xor(me, step)] = ref[...]
    points, lanes = own_ref.shape[1:]
    units = real_ref.shape[0] // X_RADIX
    half = math.sqrt(0.5)
    f = [line_ref[at] for at in range(X_RADIX)]
    a = [f[at] + f[at + 4] for at in range(4)]
    d = [f[at] - f[at + 4] for at in range(4)]
    even, odd = a[0] + a[2], a[1] + a[3]
    less, more = (d[1] - d[3]) * half, (d[1] + d[3]) * half
    groups = (
        (0, 4, even + odd, even - odd),
        (1, 7, d[0] + less, -(d[2] + more)),
        (2, 6, a[0] - a[2], -(a[1] - a[3])),
        (3, 5, d[0] - less, d[2] - more),
    )
    for at, (c, e, left, right) in enumerate(groups):
        high, low = split(jnp.concatenate([left, right], axis=1))
        top = table_ref[at, :, :points]
        product = dot(top, high) + dot(table_ref[at, :, points:], high) + dot(top, low)
        cos_c, sin_c = product[:units], product[units : 2 * units]
        cos_e, sin_e = product[2 * units : 3 * units], product[3 * units :]
        rows_c, rows_e = pl.ds(c * units, units), pl.ds(e * units, units)
        if c == 0:
            real_ref[rows_c] = cos_c[:, :lanes]
            imag_ref[rows_c] = -sin_c[:, :lanes]
            real_ref[rows_e] = cos_e[:, lanes:]
            imag_ref[rows_e] = -sin_e[:, lanes:]
        else:
            real_ref[rows_c] = cos_c[:, :lanes] + sin_c[:, lanes:]
            imag_ref[rows_c] = cos_c[:, lanes:] - sin_c[:, :lanes]
            real_ref[rows_e] = cos_e[:, :lanes] - sin_e[:, lanes:]
            imag_ref[rows_e] = -cos_e[:, lanes:] - sin_e[:, :lanes]

    count, _, rows, _ = outs[0].shape

    def place(to, carry):
        start = to // gy * (gy * PIECES) + to % gy
        for piece, out_ref in enumerate(outs):
            for row in range(rows):
                source = where_ref[(start + piece * gy) * rows + row]
                out_ref[to, 0, pl.ds(row, 1), :] = real_ref[pl.ds(source, 1), :]
                out_ref[to, 1, pl.ds(row, 1), :] = imag_ref[pl.ds(source, 1), :]
        return carry

    lax.fori_loop(0, count, place, 0)


def x_lines(me, where, fields, first, columns, others, table, gx, gy):
    _, rows, width = fields.shape
    lanes = width // columns
    kept = where.shape[0]

    def own(_, me_ref, where_ref):
        return (first + me_ref[0] // columns, 0, me_ref[0] % columns)

    whole = lambda *shape: pl.BlockSpec(shape, lambda *_: (0,) * len(shape))
    out = (gx * gy, 2, kept // (gx * gy * PIECES), lanes)
    return pl.pallas_call(
        partial(x_body, gy),
        grid_spec=pltpu.PrefetchScalarGridSpec(
            num_scalar_prefetch=2,
            grid=(1,),
            in_specs=[pl.BlockSpec((1, rows, lanes), own)]
            + [whole(rows, lanes)] * len(others)
            + [whole(*table.shape)],
            out_specs=[whole(*out)] * PIECES,
            scratch_shapes=[
                pltpu.VMEM((X_RADIX, rows, lanes), jnp.float32),
                pltpu.VMEM((kept, lanes), jnp.float32),
                pltpu.VMEM((kept, lanes), jnp.float32),
            ],
        ),
        out_shape=[jax.ShapeDtypeStruct(out, jnp.float32)] * PIECES,
        name="x_lines",
    )(me, where, fields, *others, table)


def y_body(me_ref, in_ref, twiddle_ref, table_ref, *refs):
    outs = refs[:Y_RADIX]
    high_ref, low_ref, wave_ref = refs[Y_RADIX:]
    me = me_ref[0]
    sources, _, rows, lanes = in_ref.shape
    short = table_ref.shape[1]
    columns = short // lanes
    levels = sources // (Y_RADIX * columns)
    block = levels * rows
    for level in range(levels):
        for column in range(columns):
            base = (level * columns + column) * Y_RADIX
            re = [in_ref[base + at, 0] for at in range(Y_RADIX)]
            im = [in_ref[base + at, 1] for at in range(Y_RADIX)]
            even_r, even_i, odd_r, odd_i = re[0] + re[2], im[0] + im[2], re[1] + re[3], im[1] + im[3]
            less_r, less_i, more_r, more_i = re[0] - re[2], im[0] - im[2], re[1] - re[3], im[1] - im[3]
            folded = (
                (even_r + odd_r, even_i + odd_i),
                (less_r + more_i, less_i - more_r),
                (even_r - odd_r, even_i - odd_i),
                (less_r - more_i, less_i + more_r),
            )
            span = pl.ds(column * lanes, lanes)
            for c, (real, imag) in enumerate(folded):
                if c:
                    cos = twiddle_ref[pl.ds(c, 1), span]
                    sin = twiddle_ref[pl.ds(Y_RADIX + c, 1), span]
                    real, imag = real * cos + imag * sin, imag * cos - real * sin
                for part, values in enumerate((real, imag)):
                    high, low = split(values)
                    at = pl.ds((c * 2 + part) * block + level * rows, rows)
                    high_ref[at, span] = high
                    low_ref[at, span] = low
    whole = dot(high_ref[...], table_ref[0]) + dot(low_ref[...], table_ref[0]) + dot(high_ref[...], table_ref[1])
    for c in range(Y_RADIX):
        product = whole[c * 2 * block : (c + 1) * 2 * block]
        real = product[:block, :short] + product[block:, short:]
        imag = product[block:, :short] - product[:block, short:]
        for to in range(Y_RADIX):
            piece = slice(to * (short // Y_RADIX), (to + 1) * (short // Y_RADIX))
            wave_ref[c, to, :block] = real[:, piece]
            wave_ref[c, to, block:] = imag[:, piece]
    lane = lax.broadcasted_iota(jnp.int32, (rows, LANES), 1)
    residue = lane % Y_RADIX
    for step in range(Y_RADIX):
        to = jnp.bitwise_xor(me, step)
        for part in range(2):
            for level in range(levels):
                at = pl.ds(part * block + level * rows, rows)
                pieces = [wave_ref[c, to, at, :] for c in range(Y_RADIX)]
                for tile in range(Y_RADIX):
                    index = tile * (LANES // Y_RADIX) + lane // Y_RADIX
                    value = jnp.take_along_axis(pieces[0], index, axis=1, mode="promise_in_bounds")
                    for c in range(1, Y_RADIX):
                        other = jnp.take_along_axis(pieces[c], index, axis=1, mode="promise_in_bounds")
                        value = jnp.where(residue == c, other, value)
                    outs[step][part, level, :, pl.ds(tile * LANES, LANES)] = value


def y_lines(me, spectra, twiddles, table):
    sources, _, rows, lanes = spectra.shape
    short = table.shape[1]
    levels = sources * lanes // (Y_RADIX * short)
    whole = lambda *shape: pl.BlockSpec(shape, lambda *_: (0,) * len(shape))
    out = (2, levels, rows, short)
    tall = Y_RADIX * 2 * levels * rows
    return pl.pallas_call(
        y_body,
        grid_spec=pltpu.PrefetchScalarGridSpec(
            num_scalar_prefetch=1,
            grid=(1,),
            in_specs=[whole(*spectra.shape), whole(*twiddles.shape), whole(*table.shape)],
            out_specs=[whole(*out)] * Y_RADIX,
            scratch_shapes=[
                pltpu.VMEM((tall, short), jnp.bfloat16),
                pltpu.VMEM((tall, short), jnp.bfloat16),
                pltpu.VMEM((Y_RADIX, Y_RADIX, 2 * levels * rows, short // Y_RADIX), jnp.float32),
            ],
        ),
        out_shape=[jax.ShapeDtypeStruct(out, jnp.float32)] * Y_RADIX,
        name="y_lines",
    )(me, spectra, twiddles, table)


def finish_body(me_ref, *refs):
    blocks, mask_ref, out_ref = refs[:Y_RADIX], refs[Y_RADIX], refs[-1]
    rows = blocks[0].shape[2]
    for step, ref in enumerate(blocks):
        at = pl.ds(pl.multiple_of(jnp.bitwise_xor(me_ref[0], step) * rows, 8), rows)
        weight = mask_ref[at, :].astype(jnp.float32)
        for part in range(2):
            out_ref[part, 0, at, :] = ref[part, 0] * weight


def finish(me, blocks, kept_mask, piece, stack_count, before):
    _, levels, rows, width = blocks[0].shape
    rows_out = rows * Y_RADIX
    block = pl.BlockSpec((2, 1, rows, width), lambda level, me_ref: (0, level, 0, 0))
    extra = [] if before is None else [before]
    return pl.pallas_call(
        finish_body,
        grid_spec=pltpu.PrefetchScalarGridSpec(
            num_scalar_prefetch=1,
            grid=(levels,),
            in_specs=[block] * Y_RADIX
            + [pl.BlockSpec((rows_out, width), lambda level, me_ref: (piece, 0))]
            + [pl.BlockSpec(memory_space=pl.ANY)] * len(extra),
            out_specs=pl.BlockSpec(
                (2, 1, rows_out, width), lambda level, me_ref: (0, level, piece, 0)
            ),
        ),
        out_shape=jax.ShapeDtypeStruct((2, stack_count) + kept_mask.shape, jnp.float32),
        input_output_aliases={} if before is None else {2 + Y_RADIX: 0},
        name="finish",
    )(me, *blocks, kept_mask, *extra)


def turn(values):
    lane = lax.broadcasted_iota(jnp.int32, values.shape, 1)
    rolled = pltpu.roll(values, LANES // 2, 1)
    return jnp.where(lane < LANES // 2, rolled, -rolled)


def y_first_body(scale, me_ref, own_ref, *refs):
    others = refs[: Y_RADIX - 1]
    twiddle_ref, table_ref = refs[Y_RADIX - 1 : Y_RADIX + 1]
    outs = refs[Y_RADIX + 1 : Y_RADIX + 1 + X_RADIX]
    field_ref, wave_ref = refs[Y_RADIX + 1 + X_RADIX :]
    me_x, me_y = me_ref[0], me_ref[1]
    rows, short = own_ref.shape[1:]
    half = short // 2
    field_ref[me_y] = own_ref[0]
    for step, ref in enumerate(others, 1):
        field_ref[jnp.bitwise_xor(me_y, step)] = ref[...]
    even, odd = field_ref[0] + field_ref[2], field_ref[1] + field_ref[3]
    less, more = field_ref[0] - field_ref[2], field_ref[1] - field_ref[3]
    folded = ((even + odd, None), (less, -more), (even - odd, None), (less, more))
    for c, (real, imag) in enumerate(folded):
        if c:
            cos, sin = twiddle_ref[pl.ds(c, 1), :], twiddle_ref[pl.ds(Y_RADIX + c, 1), :]
            if imag is None:
                real, imag = real * cos, -real * sin
            else:
                real, imag = real * cos + imag * sin, imag * cos - real * sin
        tall = real if imag is None else jnp.concatenate([real, imag], axis=0)
        high, low = split(tall)
        parts = []
        for span in (pl.ds(0, half), pl.ds(short, half)):
            parts.append(dot(high, table_ref[0, :, span]) + dot(low, table_ref[0, :, span]) + dot(high, table_ref[1, :, span]))
        by_cos, by_sin = parts
        if imag is None:
            point = lax.broadcasted_iota(jnp.int32, real.shape, 1)
            top = jnp.sum(jnp.where(point % 2 == 0, real, -real), axis=1, keepdims=True) * scale
            unit = lax.broadcasted_iota(jnp.int32, by_sin.shape, 1)
            wave_ref[c, 0] = by_cos
            wave_ref[c, 1] = jnp.where(unit == 0, top, -by_sin)
        else:
            wave_ref[c, 0] = by_cos[:rows] + by_sin[rows:]
            wave_ref[c, 1] = by_cos[rows:] - by_sin[:rows]
    chunk = 32

    def place(at, carry):
        span = pl.ds(pl.multiple_of(at * chunk, chunk), chunk)
        lane = lax.broadcasted_iota(jnp.int32, (chunk, LANES), 1)
        local = lane % (LANES // 2)
        for step in range(X_RADIX):
            to = jnp.bitwise_xor(me_x, step)
            index = to * (LANES // 2 // Y_RADIX) + local // Y_RADIX
            for side in range(2):
                units = pl.ds(side * LANES, LANES)
                value = None
                for c in range(Y_RADIX):
                    pair = [
                        jnp.take_along_axis(wave_ref[c, part, span, units], index, axis=1, mode="promise_in_bounds")
                        for part in range(2)
                    ]
                    both = jnp.where(lane < LANES // 2, *pair)
                    value = both if c == 0 else jnp.where(lane % Y_RADIX == c, both, value)
                outs[step][span, units] = value
        return carry

    lax.fori_loop(0, rows // chunk, place, 0)


def y_first(me, scale, fields, first, others, twiddles, table):
    _, rows, short = fields.shape
    whole = lambda *shape: pl.BlockSpec(shape, lambda *_: (0,) * len(shape))
    out = (rows, 2 * LANES)
    return pl.pallas_call(
        partial(y_first_body, scale),
        grid_spec=pltpu.PrefetchScalarGridSpec(
            num_scalar_prefetch=1,
            grid=(1,),
            in_specs=[pl.BlockSpec((1, rows, short), lambda _, me_ref: (first + me_ref[1], 0, 0))]
            + [whole(rows, short)] * len(others)
            + [whole(*twiddles.shape), whole(*table.shape)],
            out_specs=[whole(*out)] * X_RADIX,
            scratch_shapes=[
                pltpu.VMEM((Y_RADIX, rows, short), jnp.float32),
                pltpu.VMEM((Y_RADIX, 2, rows, short // 2), jnp.float32),
            ],
        ),
        out_shape=[jax.ShapeDtypeStruct(out, jnp.float32)] * X_RADIX,
        name="y_first",
    )(me, fields, *others, twiddles, table)


def x_second_body(me_ref, where_ref, *refs):
    blocks = refs[:X_RADIX]
    table_ref, out_ref, fold_ref, wave_ref = refs[X_RADIX:]
    me = me_ref[0]
    points = blocks[0].shape[0]
    units = wave_ref.shape[1] // X_RADIX
    for step, ref in enumerate(blocks):
        fold_ref[jnp.bitwise_xor(me, step)] = ref[...]
    half = math.sqrt(0.5)
    for side in range(2):
        span = pl.ds(side * LANES, LANES)
        f = [fold_ref[at, :, span] for at in range(X_RADIX)]
        a = [f[at] + f[at + 4] for at in range(4)]
        d = [f[at] - f[at + 4] for at in range(4)]
        even, odd, less, more = a[0] + a[2], a[1] + a[3], a[0] - a[2], turn(a[1] - a[3])
        across, along = turn(d[2]), turn(d[1] + d[3])
        one = (d[1] - d[3] + along) * half
        three = (along - d[1] + d[3]) * half
        folded = {
            0: even + odd,
            4: even - odd,
            2: less + more,
            6: less - more,
            1: d[0] + across + one,
            5: d[0] + across - one,
            3: d[0] - across + three,
            7: d[0] - across - three,
        }
        for c, values in folded.items():
            fold_ref[c, :, span] = values
    lane = lax.broadcasted_iota(jnp.int32, (points, 2 * LANES), 1)
    sign = jnp.where(lane % LANES < LANES // 2, 1.0, -1.0)
    lane = lax.broadcasted_iota(jnp.int32, (units, LANES), 1)
    special = jnp.logical_and(lane % (LANES // 2) == 0, me == 0)
    for at, pair in enumerate(((0, 4), (1, 7), (2, 6), (3, 5))):
        for side, c in enumerate(pair):
            data = jnp.concatenate([fold_ref[c], fold_ref[-c % X_RADIX] * sign], axis=1)
            high, low = split(data)
            rows = pl.ds(side * 2 * units, 2 * units)
            top = table_ref[at, rows, :points]
            product = dot(top, high) + dot(table_ref[at, rows, points:], high) + dot(top, low)
            plus_low, plus_high, minus_low, minus_high = (
                product[:units, piece * LANES : (piece + 1) * LANES]
                + turn(product[units:, piece * LANES : (piece + 1) * LANES])
                for piece in range(4)
            )
            rows = pl.ds(c * units, units)
            wave_ref[0, rows] = jnp.where(special, (plus_low + minus_low) * 0.5, plus_low)
            wave_ref[1, rows] = plus_high
            wave_ref[2, rows] = jnp.where(special, turn(plus_low - minus_low) * 0.5, minus_high)
            wave_ref[3, rows] = jnp.where(special, minus_high, minus_low)

    count, rows, _ = out_ref.shape
    unroll = 32

    def place(at, carry):
        to, start = at // (rows // unroll) * Y_RADIX, at % (rows // unroll) * unroll
        for row in range(unroll):
            source = where_ref[at * unroll + row]
            for piece in range(Y_RADIX):
                out_ref[to + piece, pl.ds(start + row, 1), :] = wave_ref[piece, pl.ds(source, 1), :]
        return carry

    lax.fori_loop(0, count // Y_RADIX * (rows // unroll), place, 0)


def x_second(me, where, blocks, table, gx):
    points, lanes = blocks[0].shape
    kept = where.shape[0]
    whole = lambda *shape: pl.BlockSpec(shape, lambda *_: (0,) * len(shape))
    out = (gx * Y_RADIX, kept // gx, LANES)
    return pl.pallas_call(
        x_second_body,
        grid_spec=pltpu.PrefetchScalarGridSpec(
            num_scalar_prefetch=2,
            grid=(1,),
            in_specs=[whole(points, lanes)] * X_RADIX + [whole(*table.shape)],
            out_specs=whole(*out),
            scratch_shapes=[
                pltpu.VMEM((X_RADIX, points, lanes), jnp.float32),
                pltpu.VMEM((Y_RADIX, kept, LANES), jnp.float32),
            ],
        ),
        out_shape=jax.ShapeDtypeStruct(out, jnp.float32),
        name="x_second",
    )(me, where, *blocks, table)


def finish_second_body(me_ref, in_ref, mask_ref, before_ref, out_ref):
    mirrored = me_ref[0] >= Y_RADIX // 2
    rows = mask_ref.shape[0]
    chunk = 32

    def place(at, carry):
        span = pl.ds(pl.multiple_of(at * chunk, chunk), chunk)
        lane = lax.broadcasted_iota(jnp.int32, (chunk, LANES), 1)
        left = lane < LANES // 2
        index = jnp.where(mirrored, (LANES - lane) % LANES, lane)
        for tile in range(Y_RADIX):
            body = jnp.where(mirrored, Y_RADIX - 1 - tile, tile)
            head = jnp.where(mirrored, (Y_RADIX - tile) % Y_RADIX, tile)
            here, there = in_ref[2 * body, 0, span, :], in_ref[2 * body + 1, 0, span, :]
            start = in_ref[2 * head, 0, span, :]
            real = jnp.where(left, here, pltpu.roll(there, LANES // 2, 1))
            imag = jnp.where(left, pltpu.roll(here, LANES // 2, 1), there)
            lanes = pl.ds(tile * LANES, LANES)
            weight = mask_ref[span, lanes].astype(jnp.float32)
            for part, (values, edge) in enumerate(((real, start), (imag, pltpu.roll(start, LANES // 2, 1)))):
                values = jnp.take_along_axis(values, index, axis=1, mode="promise_in_bounds")
                out_ref[part, 0, span, lanes] = jnp.where(lane == 0, edge, values) * weight
        return carry

    lax.fori_loop(0, rows // chunk, place, 0)


def finish_second(me, blocks, kept_mask, first, before):
    gx, levels, rows, lanes = blocks.shape
    return pl.pallas_call(
        finish_second_body,
        grid_spec=pltpu.PrefetchScalarGridSpec(
            num_scalar_prefetch=1,
            grid=(levels,),
            in_specs=[
                pl.BlockSpec((gx, 1, rows, lanes), lambda level, me_ref: (0, level, 0, 0)),
                pl.BlockSpec(kept_mask.shape, lambda level, me_ref: (0, 0)),
                pl.BlockSpec(memory_space=pl.ANY),
            ],
            out_specs=pl.BlockSpec(
                (2, 1) + kept_mask.shape, lambda level, me_ref: (0, first + level, 0, 0)
            ),
        ),
        out_shape=jax.ShapeDtypeStruct(before.shape, jnp.float32),
        input_output_aliases={3: 0},
        name="finish_second",
    )(me, blocks, kept_mask, before)


def exchange(blocks, axis, size):
    return [
        lax.ppermute(block, axis, [(at, at ^ step) for at in range(size)])
        for step, block in enumerate(blocks, 1)
    ]


def fast_shards(gx, gy, nx, ny, fields, wave_order, kept_mask):
    stack_count = fields.shape[0]
    kept = wave_order.shape[0]
    levels = stack_count // HALVES
    columns = gx // levels
    me_x, me_y = lax.axis_index("gx"), lax.axis_index("gy")
    zero = me_x // gx
    x_me, y_me = me_x.reshape(1).astype(jnp.int32), me_y.reshape(1).astype(jnp.int32)
    where = (wave_order % X_RADIX) * (kept // X_RADIX) + wave_order // X_RADIX
    both_me = jnp.concatenate([x_me, y_me])
    scale = 1.0 / math.sqrt(nx * ny)
    whole = ("gx", "gy")
    second = levels
    fields_second = exchange(pack(y_me, fields, second, 1), "gy", gy)
    lines = exchange(pack(x_me, fields, 0, columns), "gx", gx)
    tables = x_table(nx, kept, zero), y_table(ny, scale, zero), y_twiddles(ny, zero)
    table_x, table_y, twiddles = lax.optimization_barrier(tables)
    spectra = x_lines(x_me, where, fields, 0, columns, lines, table_x, gx, gy)
    spectra = list(spectra)
    for piece in range(PIECES):
        spectra[piece] = lax.all_to_all(spectra[piece], whole, split_axis=0, concat_axis=0, tiled=True)
    half_waves = y_first(both_me, scale, fields, second, fields_second, twiddles, table_y)
    half_waves = [half_waves[0]] + exchange(half_waves[1:], "gx", gx)
    owned = x_second(x_me, where, half_waves, table_x, gx)
    owned = lax.all_to_all(owned, whole, split_axis=0, concat_axis=0, tiled=True)
    result = None
    for piece in range(PIECES):
        waves = y_lines(y_me, spectra[piece], twiddles, table_y)
        waves = [waves[0]] + exchange(waves[1:], "gy", gy)
        if piece == PIECES - 1:
            owned = owned.reshape((gx, gy) + owned.shape[1:])
            result = finish_second(y_me, owned, kept_mask, second, result)
        result = finish(y_me, waves, kept_mask, piece, stack_count, result)
    return result


def wave_angles(wave_ids, points, period):
    phases = wave_ids[:, None] * points[None, :] % period
    angles = phases.astype(jnp.float32) * (2.0 * math.pi / period)
    return (jnp.cos(angles), jnp.sin(angles))


def x_terms(cos_table, sin_table, values):
    stack_count, x_count, y_count = values.shape
    waves = cos_table.shape[0]
    table = jnp.concatenate([cos_table, -sin_table], axis=0)
    flat = jnp.transpose(values, (1, 0, 2)).reshape(x_count, stack_count * y_count)
    product = jnp.dot(
        table, flat, precision=lax.Precision.HIGHEST, preferred_element_type=jnp.float32
    )
    product = product.reshape(2, waves, stack_count, y_count)
    return jnp.transpose(product, (1, 0, 2, 3))


def y_terms(cos_table, sin_table, spectra):
    rows, parts, stack_count, y_count = spectra.shape
    waves = cos_table.shape[0]
    table = jnp.concatenate([cos_table, sin_table], axis=0)
    flat = spectra.reshape(rows * parts * stack_count, y_count)
    product = jnp.dot(
        flat, table.T, precision=lax.Precision.HIGHEST, preferred_element_type=jnp.float32
    )
    product = product.reshape(rows, parts, stack_count, 2, waves)
    real_part = product[:, 0, :, 0] + product[:, 1, :, 1]
    imag_part = product[:, 1, :, 0] - product[:, 0, :, 1]
    return jnp.stack([real_part, imag_part], axis=1)


def plain_shards(nx, ny, fields, wave_order, kept_mask):
    x_every = jnp.arange(nx, dtype=jnp.int32)
    x_cos, x_sin = wave_angles(wave_order, x_every, nx)
    partial_terms = x_terms(
        x_cos, x_sin, lax.all_to_all(fields, "gx", split_axis=2, concat_axis=1, tiled=True)
    )
    spectra = lax.all_to_all(partial_terms, "gx", split_axis=0, concat_axis=3, tiled=True)
    y_every = jnp.arange(ny, dtype=jnp.int32)
    y_cos, y_sin = wave_angles(y_every, y_every, ny)
    y_spectra = y_terms(
        y_cos, y_sin, lax.all_to_all(spectra, "gy", split_axis=0, concat_axis=3, tiled=True)
    )
    result = lax.all_to_all(y_spectra, "gy", split_axis=3, concat_axis=0, tiled=True)
    weight = kept_mask.astype(jnp.float32) * (1.0 / math.sqrt(nx * ny))
    return jnp.transpose(result, (1, 2, 0, 3)) * weight[None, None]


def fits(gx, gy, stack_count, nx, ny, kept):
    levels = stack_count // HALVES
    if gx != X_RADIX or gy != Y_RADIX or levels != gy or stack_count % HALVES:
        return False
    lanes = ny // gy // (gx // levels)
    return (
        lanes % LANES == 0
        and ny == Y_RADIX * Y_RADIX * LANES
        and nx % (X_RADIX * LANES) == 0
        and kept % (X_RADIX * LANES) == 0
        and kept <= nx
        and kept // (gx * gy) % (16 * PIECES) == 0
    )


def solution(mesh):
    gx, gy = mesh.shape["gx"], mesh.shape["gy"]

    def call(fields, wave_order, kept_mask):
        stack_count, nx, ny = fields.shape
        if fits(gx, gy, stack_count, nx, ny, wave_order.shape[0]):
            body = partial(fast_shards, gx, gy, nx, ny)
        else:
            body = partial(plain_shards, nx, ny)
        return jax.shard_map(
            body,
            mesh=mesh,
            in_specs=(P(None, "gx", "gy"), P(), P("gx", "gy")),
            out_specs=P(None, None, "gx", "gy"),
            check_vma=False,
        )(fields, wave_order, kept_mask)

    return call
```

```python
import math
from functools import partial

import jax
import jax.numpy as jnp
from jax import lax
from jax.experimental import pallas as pl
from jax.experimental.pallas import tpu as pltpu
from jax.sharding import PartitionSpec as P


X_RADIX = 8
Y_RADIX = 4
HALVES = 2
PIECES = 2
LANES = 128


def roots(numbers, period):
    angles = (numbers % period).astype(jnp.float32) * (2.0 * math.pi / period)
    return jnp.cos(angles), jnp.sin(angles)


def two_parts(values):
    high = lax.reduce_precision(values, 8, 7)
    return high.astype(jnp.bfloat16), (values - high).astype(jnp.bfloat16)


def x_table(period, kept, zero):
    points = jnp.arange(period // X_RADIX, dtype=jnp.int32) + zero
    units = jnp.arange(kept // X_RADIX, dtype=jnp.int32) * X_RADIX
    pairs = jnp.array([[0, 4], [1, 7], [2, 6], [3, 5]], dtype=jnp.int32)
    waves = pairs[:, :, None] + units[None, None, :]
    cos, sin = roots(waves[..., None] * points, period)
    table = jnp.stack([cos, sin], axis=2).reshape(4, 4 * units.shape[0], points.shape[0])
    return jnp.concatenate(two_parts(table), axis=2)


def y_table(period, scale, zero):
    short = period // Y_RADIX
    ids = jnp.arange(short, dtype=jnp.int32) + zero
    cos, sin = roots(ids[:, None] * ids[None, :], short)
    half = short // 2
    table = jnp.concatenate([cos[:, :half], sin[:, :half], cos[:, half:], sin[:, half:]], axis=1)
    return jnp.stack(two_parts(table * scale))


def y_twiddles(period, zero):
    ids = jnp.arange(period // Y_RADIX, dtype=jnp.int32) + zero
    cos, sin = roots(jnp.arange(Y_RADIX, dtype=jnp.int32)[:, None] * ids[None, :], period)
    return jnp.concatenate([cos, sin], axis=0)


IN_VMEM = pl.BlockSpec(memory_space=pltpu.VMEM)
IN_HBM = pl.BlockSpec(memory_space=pltpu.HBM)
LIMIT = pltpu.CompilerParams(vmem_limit_bytes=32 << 20)


def in_hbm(array):
    return pltpu.with_memory_space_constraint(array, pltpu.HBM)


def on_chip(*arrays):
    return [pltpu.with_memory_space_constraint(array, pltpu.VMEM) for array in arrays]


def dot(left, right):
    return jnp.dot(left, right, preferred_element_type=jnp.float32)


def split(values):
    high = values.astype(jnp.bfloat16)
    return high, (values - high.astype(jnp.float32)).astype(jnp.bfloat16)


def copy_all(pairs, semaphore):
    copies = [
        pltpu.make_async_copy(source, target, semaphore.at[at])
        for at, (source, target) in enumerate(pairs)
    ]
    for copy in copies:
        copy.start()
    return copies


def column_block(fields_ref, first, columns, to, lanes):
    if columns == 1:
        return fields_ref.at[first + to]
    start = pl.multiple_of(to % columns * lanes, LANES)
    return fields_ref.at[first + to // columns, :, pl.ds(start, lanes)]


def pack_body(first, columns, me_ref, fields_ref, *refs):
    outs, semaphore = refs[:-1], refs[-1]
    lanes = outs[0].shape[1]
    pairs = [
        (column_block(fields_ref, first, columns, jnp.bitwise_xor(me_ref[0], step), lanes), out)
        for step, out in enumerate(outs, 1)
    ]
    for copy in copy_all(pairs, semaphore):
        copy.wait()


def pack(me, fields, first, columns):
    stack_count, rows, width = fields.shape
    lanes = width // columns
    count = (stack_count // HALVES) * columns - 1
    return pl.pallas_call(
        partial(pack_body, first, columns),
        grid_spec=pltpu.PrefetchScalarGridSpec(
            num_scalar_prefetch=1,
            grid=(1,),
            in_specs=[IN_HBM],
            out_specs=[IN_VMEM] * count,
            scratch_shapes=[pltpu.SemaphoreType.DMA((count,))],
        ),
        out_shape=[pltpu.HBM((rows, lanes), jnp.float32)] * count,
        compiler_params=LIMIT,
        name="pack",
    )(me, in_hbm(fields))


def x_body(gy, first, columns, me_ref, where_ref, fields_ref, *refs):
    others, table_ref = refs[: X_RADIX - 1], refs[X_RADIX - 1]
    outs = refs[X_RADIX : X_RADIX + PIECES]
    line_ref, real_ref, imag_ref, semaphore = refs[X_RADIX + PIECES :]
    me = me_ref[0]
    points, lanes = line_ref.shape[1:]
    own = copy_all([(column_block(fields_ref, first, columns, me, lanes), line_ref.at[me])], semaphore)
    for step, ref in enumerate(others, 1):
        line_ref[jnp.bitwise_xor(me, step)] = ref[...]
    own[0].wait()
    units = real_ref.shape[0] // X_RADIX
    half = math.sqrt(0.5)
    f = [line_ref[at] for at in range(X_RADIX)]
    a = [f[at] + f[at + 4] for at in range(4)]
    d = [f[at] - f[at + 4] for at in range(4)]
    even, odd = a[0] + a[2], a[1] + a[3]
    less, more = (d[1] - d[3]) * half, (d[1] + d[3]) * half
    groups = (
        (0, 4, even + odd, even - odd),
        (1, 7, d[0] + less, -(d[2] + more)),
        (2, 6, a[0] - a[2], -(a[1] - a[3])),
        (3, 5, d[0] - less, d[2] - more),
    )
    for at, (c, e, left, right) in enumerate(groups):
        high, low = split(jnp.concatenate([left, right], axis=1))
        top = table_ref[at, :, :points]
        product = dot(top, high) + dot(table_ref[at, :, points:], high) + dot(top, low)
        cos_c, sin_c = product[:units], product[units : 2 * units]
        cos_e, sin_e = product[2 * units : 3 * units], product[3 * units :]
        rows_c, rows_e = pl.ds(c * units, units), pl.ds(e * units, units)
        if c == 0:
            real_ref[rows_c] = cos_c[:, :lanes]
            imag_ref[rows_c] = -sin_c[:, :lanes]
            real_ref[rows_e] = cos_e[:, lanes:]
            imag_ref[rows_e] = -sin_e[:, lanes:]
        else:
            real_ref[rows_c] = cos_c[:, :lanes] + sin_c[:, lanes:]
            imag_ref[rows_c] = cos_c[:, lanes:] - sin_c[:, :lanes]
            real_ref[rows_e] = cos_e[:, :lanes] - sin_e[:, lanes:]
            imag_ref[rows_e] = -cos_e[:, lanes:] - sin_e[:, :lanes]

    count, _, rows, _ = outs[0].shape

    def place(to, carry):
        start = to // gy * (gy * PIECES) + to % gy
        for piece, out_ref in enumerate(outs):
            for row in range(rows):
                source = where_ref[(start + piece * gy) * rows + row]
                out_ref[to, 0, pl.ds(row, 1), :] = real_ref[pl.ds(source, 1), :]
                out_ref[to, 1, pl.ds(row, 1), :] = imag_ref[pl.ds(source, 1), :]
        return carry

    lax.fori_loop(0, count, place, 0)


def x_lines(me, where, fields, first, columns, others, table, gx, gy):
    rows, lanes = others[0].shape
    kept = where.shape[0]
    out = (gx * gy, 2, kept // (gx * gy * PIECES), lanes)
    return pl.pallas_call(
        partial(x_body, gy, first, columns),
        grid_spec=pltpu.PrefetchScalarGridSpec(
            num_scalar_prefetch=2,
            grid=(1,),
            in_specs=[IN_HBM] + [IN_VMEM] * X_RADIX,
            out_specs=[IN_VMEM] * PIECES,
            scratch_shapes=[
                pltpu.VMEM((X_RADIX, rows, lanes), jnp.float32),
                pltpu.VMEM((kept, lanes), jnp.float32),
                pltpu.VMEM((kept, lanes), jnp.float32),
                pltpu.SemaphoreType.DMA((1,)),
            ],
        ),
        out_shape=[pltpu.HBM(out, jnp.float32)] * PIECES,
        compiler_params=LIMIT,
        name="x_lines",
    )(me, where, in_hbm(fields), *on_chip(*others, table))


def y_body(me_ref, in_ref, twiddle_ref, table_ref, *refs):
    outs = refs[:Y_RADIX]
    high_ref, low_ref, wave_ref = refs[Y_RADIX:]
    me = me_ref[0]
    sources, _, rows, lanes = in_ref.shape
    short = table_ref.shape[1]
    columns = short // lanes
    levels = sources // (Y_RADIX * columns)
    block = levels * rows
    for level in range(levels):
        for column in range(columns):
            base = (level * columns + column) * Y_RADIX
            re = [in_ref[base + at, 0] for at in range(Y_RADIX)]
            im = [in_ref[base + at, 1] for at in range(Y_RADIX)]
            even_r, even_i, odd_r, odd_i = re[0] + re[2], im[0] + im[2], re[1] + re[3], im[1] + im[3]
            less_r, less_i, more_r, more_i = re[0] - re[2], im[0] - im[2], re[1] - re[3], im[1] - im[3]
            folded = (
                (even_r + odd_r, even_i + odd_i),
                (less_r + more_i, less_i - more_r),
                (even_r - odd_r, even_i - odd_i),
                (less_r - more_i, less_i + more_r),
            )
            span = pl.ds(column * lanes, lanes)
            for c, (real, imag) in enumerate(folded):
                if c:
                    cos = twiddle_ref[pl.ds(c, 1), span]
                    sin = twiddle_ref[pl.ds(Y_RADIX + c, 1), span]
                    real, imag = real * cos + imag * sin, imag * cos - real * sin
                for part, values in enumerate((real, imag)):
                    high, low = split(values)
                    at = pl.ds((c * 2 + part) * block + level * rows, rows)
                    high_ref[at, span] = high
                    low_ref[at, span] = low
    whole = dot(high_ref[...], table_ref[0]) + dot(low_ref[...], table_ref[0]) + dot(high_ref[...], table_ref[1])
    for c in range(Y_RADIX):
        product = whole[c * 2 * block : (c + 1) * 2 * block]
        for to in range(Y_RADIX):
            start = (to // 2 * Y_RADIX + to % 2) * LANES
            by_cos, by_sin = slice(start, start + LANES), slice(start + 2 * LANES, start + 3 * LANES)
            wave_ref[c, to, :block] = product[:block, by_cos] + product[block:, by_sin]
            wave_ref[c, to, block:] = product[block:, by_cos] - product[:block, by_sin]
    lane = lax.broadcasted_iota(jnp.int32, (rows, LANES), 1)
    residue = lane % Y_RADIX
    for step in range(Y_RADIX):
        to = jnp.bitwise_xor(me, step)
        for part in range(2):
            for level in range(levels):
                at = pl.ds(part * block + level * rows, rows)
                pieces = [wave_ref[c, to, at, :] for c in range(Y_RADIX)]
                for tile in range(Y_RADIX):
                    index = tile * (LANES // Y_RADIX) + lane // Y_RADIX
                    value = jnp.take_along_axis(pieces[0], index, axis=1, mode="promise_in_bounds")
                    for c in range(1, Y_RADIX):
                        other = jnp.take_along_axis(pieces[c], index, axis=1, mode="promise_in_bounds")
                        value = jnp.where(residue == c, other, value)
                    outs[step][part, level, :, pl.ds(tile * LANES, LANES)] = value


def y_lines(me, spectra, twiddles, table):
    sources, _, rows, lanes = spectra.shape
    short = table.shape[1]
    levels = sources * lanes // (Y_RADIX * short)
    out = (2, levels, rows, short)
    tall = Y_RADIX * 2 * levels * rows
    return pl.pallas_call(
        y_body,
        grid_spec=pltpu.PrefetchScalarGridSpec(
            num_scalar_prefetch=1,
            grid=(1,),
            in_specs=[IN_VMEM] * 3,
            out_specs=[IN_VMEM] * Y_RADIX,
            scratch_shapes=[
                pltpu.VMEM((tall, short), jnp.bfloat16),
                pltpu.VMEM((tall, short), jnp.bfloat16),
                pltpu.VMEM((Y_RADIX, Y_RADIX, 2 * levels * rows, short // Y_RADIX), jnp.float32),
            ],
        ),
        out_shape=[pltpu.HBM(out, jnp.float32)] * Y_RADIX,
        compiler_params=LIMIT,
        name="y_lines",
    )(me, spectra, twiddles, table)


def finish_body(piece, me_ref, *refs):
    blocks, mask_ref, out_ref = refs[:Y_RADIX], refs[Y_RADIX], refs[-3]
    out_buffer, out_semaphore = refs[-2:]
    _, levels, rows, _ = blocks[0].shape
    rows_out = rows * Y_RADIX
    leaving = []
    for level in range(levels):
        for step in range(Y_RADIX):
            at = pl.ds(pl.multiple_of(jnp.bitwise_xor(me_ref[0], step) * rows, rows), rows)
            weight = mask_ref[at, :].astype(jnp.float32)
            for part in range(2):
                out_buffer[level, part, at, :] = blocks[step][part, level] * weight
        target = out_ref.at[:, level, pl.ds(piece * rows_out, rows_out), :]
        leaving += copy_all([(out_buffer.at[level], target)], out_semaphore.at[level])
    for copy in leaving:
        copy.wait()


def finish(me, blocks, kept_mask, piece, stack_count, before):
    _, levels, rows, width = blocks[0].shape
    rows_out = rows * Y_RADIX
    extra = [] if before is None else [before]
    return pl.pallas_call(
        partial(finish_body, piece),
        grid_spec=pltpu.PrefetchScalarGridSpec(
            num_scalar_prefetch=1,
            grid=(1,),
            in_specs=[IN_VMEM] * Y_RADIX
            + [pl.BlockSpec((rows_out, width), lambda *_: (piece, 0))]
            + [IN_HBM] * len(extra),
            out_specs=IN_HBM,
            scratch_shapes=[
                pltpu.VMEM((levels, 2, rows_out, width), jnp.float32),
                pltpu.SemaphoreType.DMA((levels, 1)),
            ],
        ),
        out_shape=jax.ShapeDtypeStruct((2, stack_count) + kept_mask.shape, jnp.float32),
        input_output_aliases={} if before is None else {2 + Y_RADIX: 0},
        compiler_params=LIMIT,
        name="finish",
    )(me, in_hbm(blocks[0]), *on_chip(*blocks[1:]), kept_mask, *extra)


def turn(values):
    lane = lax.broadcasted_iota(jnp.int32, values.shape, 1)
    rolled = pltpu.roll(values, LANES // 2, 1)
    return jnp.where(lane < LANES // 2, rolled, -rolled)


def y_first_body(scale, first, me_ref, fields_ref, *refs):
    others = refs[: Y_RADIX - 1]
    twiddle_ref, table_ref = refs[Y_RADIX - 1 : Y_RADIX + 1]
    outs = refs[Y_RADIX + 1 : Y_RADIX + 1 + X_RADIX]
    field_ref, wave_ref, semaphore = refs[Y_RADIX + 1 + X_RADIX :]
    me_x, me_y = me_ref[0], me_ref[1]
    _, rows, short = field_ref.shape
    half = short // 2
    own = copy_all([(column_block(fields_ref, first, 1, me_y, short), field_ref.at[me_y])], semaphore)
    for step, ref in enumerate(others, 1):
        field_ref[jnp.bitwise_xor(me_y, step)] = ref[...]
    own[0].wait()
    even, odd = field_ref[0] + field_ref[2], field_ref[1] + field_ref[3]
    less, more = field_ref[0] - field_ref[2], field_ref[1] - field_ref[3]
    folded = ((even + odd, None), (less, -more), (even - odd, None), (less, more))
    for c, (real, imag) in enumerate(folded):
        if c:
            cos, sin = twiddle_ref[pl.ds(c, 1), :], twiddle_ref[pl.ds(Y_RADIX + c, 1), :]
            if imag is None:
                real, imag = real * cos, -real * sin
            else:
                real, imag = real * cos + imag * sin, imag * cos - real * sin
        tall = real if imag is None else jnp.concatenate([real, imag], axis=0)
        high, low = split(tall)
        top, bottom = table_ref[0, :, :short], table_ref[1, :, :short]
        product = dot(high, top) + dot(low, top) + dot(high, bottom)
        by_cos, by_sin = product[:, :half], product[:, half:]
        if imag is None:
            point = lax.broadcasted_iota(jnp.int32, real.shape, 1)
            top = jnp.sum(jnp.where(point % 2 == 0, real, -real), axis=1, keepdims=True) * scale
            unit = lax.broadcasted_iota(jnp.int32, by_sin.shape, 1)
            wave_ref[c] = by_cos
            wave_ref[Y_RADIX + c] = jnp.where(unit == 0, top, -by_sin)
        else:
            wave_ref[c] = by_cos[:rows] + by_sin[rows:]
            wave_ref[Y_RADIX + c] = by_cos[rows:] - by_sin[:rows]
    chunk, group = 32, LANES // X_RADIX

    def place(at, carry):
        span = pl.ds(pl.multiple_of(at * chunk, chunk), chunk)
        lane = lax.broadcasted_iota(jnp.int32, (chunk, LANES), 1)
        for side in range(2):
            units = pl.ds(side * LANES, LANES)
            tiles = [wave_ref[number, span, units] for number in range(X_RADIX)]
            for bit in (1, 2, 4):
                upper = lane // (group * bit) % 2 == 1
                for low in range(X_RADIX):
                    if low & bit:
                        continue
                    one, two = tiles[low], tiles[low + bit]
                    tiles[low] = jnp.where(upper, pltpu.roll(two, group * bit, 1), one)
                    tiles[low + bit] = jnp.where(upper, two, pltpu.roll(one, LANES - group * bit, 1))
            for number, tile in enumerate(tiles):
                wave_ref[number, span, units] = tile
        return carry

    lax.fori_loop(0, rows // chunk, place, 0)
    for step, out in enumerate(outs):
        out[...] = wave_ref[jnp.bitwise_xor(me_x, step)]


def y_first(me, scale, fields, first, others, twiddles, table):
    rows, short = others[0].shape
    out = (rows, 2 * LANES)
    return pl.pallas_call(
        partial(y_first_body, scale, first),
        grid_spec=pltpu.PrefetchScalarGridSpec(
            num_scalar_prefetch=1,
            grid=(1,),
            in_specs=[IN_HBM] + [IN_VMEM] * (Y_RADIX + 1),
            out_specs=[IN_VMEM] * X_RADIX,
            scratch_shapes=[
                pltpu.VMEM((Y_RADIX, rows, short), jnp.float32),
                pltpu.VMEM((X_RADIX, rows, 2 * LANES), jnp.float32),
                pltpu.SemaphoreType.DMA((1,)),
            ],
        ),
        out_shape=[pltpu.HBM(out, jnp.float32)] * X_RADIX,
        compiler_params=LIMIT,
        name="y_first",
    )(me, in_hbm(fields), *on_chip(*others), twiddles, table)


def x_second_body(me_ref, where_ref, *refs):
    blocks = refs[:X_RADIX]
    table_ref, out_ref, fold_ref, wave_ref = refs[X_RADIX:]
    me = me_ref[0]
    points = blocks[0].shape[0]
    units = wave_ref.shape[1] // X_RADIX
    for step, ref in enumerate(blocks):
        fold_ref[jnp.bitwise_xor(me, step)] = ref[...]
    half = math.sqrt(0.5)
    for side in range(2):
        span = pl.ds(side * LANES, LANES)
        f = [fold_ref[at, :, span] for at in range(X_RADIX)]
        a = [f[at] + f[at + 4] for at in range(4)]
        d = [f[at] - f[at + 4] for at in range(4)]
        even, odd, less, more = a[0] + a[2], a[1] + a[3], a[0] - a[2], turn(a[1] - a[3])
        across, along = turn(d[2]), turn(d[1] + d[3])
        one = (d[1] - d[3] + along) * half
        three = (along - d[1] + d[3]) * half
        folded = {
            0: even + odd,
            4: even - odd,
            2: less + more,
            6: less - more,
            1: d[0] + across + one,
            5: d[0] + across - one,
            3: d[0] - across + three,
            7: d[0] - across - three,
        }
        for c, values in folded.items():
            fold_ref[c, :, span] = values
    lane = lax.broadcasted_iota(jnp.int32, (points, 2 * LANES), 1)
    sign = jnp.where(lane % LANES < LANES // 2, 1.0, -1.0)
    lane = lax.broadcasted_iota(jnp.int32, (units, LANES), 1)
    special = jnp.logical_and(lane % (LANES // 2) == 0, me == 0)
    for at, pair in enumerate(((0, 4), (1, 7), (2, 6), (3, 5))):
        for side, c in enumerate(pair):
            data = jnp.concatenate([fold_ref[c], fold_ref[-c % X_RADIX] * sign], axis=1)
            high, low = split(data)
            rows = pl.ds(side * 2 * units, 2 * units)
            top = table_ref[at, rows, :points]
            product = dot(top, high) + dot(table_ref[at, rows, points:], high) + dot(top, low)
            plus_low, plus_high, minus_low, minus_high = (
                product[:units, piece * LANES : (piece + 1) * LANES]
                + turn(product[units:, piece * LANES : (piece + 1) * LANES])
                for piece in range(4)
            )
            rows = pl.ds(c * units, units)
            wave_ref[0, rows] = jnp.where(special, (plus_low + minus_low) * 0.5, plus_low)
            wave_ref[1, rows] = plus_high
            wave_ref[2, rows] = jnp.where(special, turn(plus_low - minus_low) * 0.5, minus_high)
            wave_ref[3, rows] = jnp.where(special, minus_high, minus_low)

    count, rows, _ = out_ref.shape
    unroll = 32

    def place(at, carry):
        to, start = at // (rows // unroll) * Y_RADIX, at % (rows // unroll) * unroll
        for row in range(unroll):
            source = where_ref[at * unroll + row]
            for piece in range(Y_RADIX):
                out_ref[to + piece, pl.ds(start + row, 1), :] = wave_ref[piece, pl.ds(source, 1), :]
        return carry

    lax.fori_loop(0, count // Y_RADIX * (rows // unroll), place, 0)


def x_second(me, where, blocks, table, gx):
    points, lanes = blocks[0].shape
    kept = where.shape[0]
    out = (gx * Y_RADIX, kept // gx, LANES)
    return pl.pallas_call(
        x_second_body,
        grid_spec=pltpu.PrefetchScalarGridSpec(
            num_scalar_prefetch=2,
            grid=(1,),
            in_specs=[IN_VMEM] * (X_RADIX + 1),
            out_specs=IN_VMEM,
            scratch_shapes=[
                pltpu.VMEM((X_RADIX, points, lanes), jnp.float32),
                pltpu.VMEM((Y_RADIX, kept, LANES), jnp.float32),
            ],
        ),
        out_shape=pltpu.HBM(out, jnp.float32),
        compiler_params=LIMIT,
        name="x_second",
    )(me, where, in_hbm(blocks[0]), *on_chip(*blocks[1:]), table)


def finish_second_body(first, me_ref, blocks_ref, mask_ref, before_ref, out_ref, *refs):
    out_buffer, out_semaphore = refs
    mirrored = me_ref[0] >= Y_RADIX // 2
    _, levels, rows, _ = blocks_ref.shape
    chunk, group = 32, LANES // X_RADIX

    def place(level, at):
        span = pl.ds(pl.multiple_of(at * chunk, chunk), chunk)
        lane = lax.broadcasted_iota(jnp.int32, (chunk, LANES), 1)
        left = lane < LANES // 2
        wanted = jnp.where(mirrored, (LANES - lane) % LANES, lane)
        local = wanted % (LANES // 2)
        index = wanted - local + local % Y_RADIX * group + local // Y_RADIX
        for tile in range(Y_RADIX):
            body = jnp.where(mirrored, Y_RADIX - 1 - tile, tile)
            head = jnp.where(mirrored, (Y_RADIX - tile) % Y_RADIX, tile)
            here, there = blocks_ref[2 * body, level, span, :], blocks_ref[2 * body + 1, level, span, :]
            start = blocks_ref[2 * head, level, span, :]
            real = jnp.where(left, here, pltpu.roll(there, LANES // 2, 1))
            imag = jnp.where(left, pltpu.roll(here, LANES // 2, 1), there)
            lanes = pl.ds(tile * LANES, LANES)
            weight = mask_ref[span, lanes].astype(jnp.float32)
            for part, (values, edge) in enumerate(((real, start), (imag, pltpu.roll(start, LANES // 2, 1)))):
                values = jnp.take_along_axis(values, index, axis=1, mode="promise_in_bounds")
                out_buffer[level, part, span, lanes] = jnp.where(lane == 0, edge, values) * weight

    leaving = []
    for level in range(levels):

        def step(at, carry):
            place(level, at)
            return carry

        lax.fori_loop(0, rows // chunk, step, 0)
        leaving += copy_all([(out_buffer.at[level], out_ref.at[:, first + level])], out_semaphore.at[level])
    for copy in leaving:
        copy.wait()


def finish_second(me, blocks, kept_mask, first, before):
    _, levels, _, _ = blocks.shape
    return pl.pallas_call(
        partial(finish_second_body, first),
        grid_spec=pltpu.PrefetchScalarGridSpec(
            num_scalar_prefetch=1,
            grid=(1,),
            in_specs=[IN_VMEM, IN_VMEM, IN_HBM],
            out_specs=IN_HBM,
            scratch_shapes=[
                pltpu.VMEM((levels, 2) + kept_mask.shape, jnp.float32),
                pltpu.SemaphoreType.DMA((levels, 1)),
            ],
        ),
        out_shape=jax.ShapeDtypeStruct(before.shape, jnp.float32),
        input_output_aliases={3: 0},
        compiler_params=LIMIT,
        name="finish_second",
    )(me, *on_chip(blocks), kept_mask, before)


def exchange(blocks, axis, size):
    arrived = {}
    for step in sorted(range(1, size), key=lambda step: (step < size // 2, step)):
        pairs = [(at, at ^ step) for at in range(size)]
        arrived[step] = lax.ppermute(blocks[step - 1], axis, pairs)
    return [arrived[step] for step in range(1, size)]


def fast_shards(gx, gy, nx, ny, fields, wave_order, kept_mask):
    stack_count = fields.shape[0]
    kept = wave_order.shape[0]
    levels = stack_count // HALVES
    columns = gx // levels
    me_x, me_y = lax.axis_index("gx"), lax.axis_index("gy")
    zero = me_x // gx
    x_me, y_me = me_x.reshape(1).astype(jnp.int32), me_y.reshape(1).astype(jnp.int32)
    where = (wave_order % X_RADIX) * (kept // X_RADIX) + wave_order // X_RADIX
    both_me = jnp.concatenate([x_me, y_me])
    scale = 1.0 / math.sqrt(nx * ny)
    whole = ("gx", "gy")
    second = levels
    fields_second = exchange(pack(y_me, fields, second, 1), "gy", gy)
    lines = exchange(pack(x_me, fields, 0, columns), "gx", gx)
    tables = x_table(nx, kept, zero), y_table(ny, scale, zero), y_twiddles(ny, zero)
    table_x, table_y, twiddles = lax.optimization_barrier(tables)
    spectra = x_lines(x_me, where, fields, 0, columns, lines, table_x, gx, gy)
    spectra = list(spectra)
    for piece in range(PIECES):
        spectra[piece] = lax.all_to_all(spectra[piece], whole, split_axis=0, concat_axis=0, tiled=True)
    half_waves = y_first(both_me, scale, fields, second, fields_second, twiddles, table_y)
    half_waves = [half_waves[0]] + exchange(half_waves[1:], "gx", gx)
    owned = x_second(x_me, where, half_waves, table_x, gx)
    owned = lax.all_to_all(owned, whole, split_axis=0, concat_axis=0, tiled=True)
    result = None
    for piece in range(PIECES):
        waves = y_lines(y_me, spectra[piece], twiddles, table_y)
        waves = [waves[0]] + exchange(waves[1:], "gy", gy)
        if piece == PIECES - 1:
            owned = owned.reshape((gx, gy) + owned.shape[1:])
            result = finish_second(y_me, owned, kept_mask, second, result)
        result = finish(y_me, waves, kept_mask, piece, stack_count, result)
    return result


def wave_angles(wave_ids, points, period):
    phases = wave_ids[:, None] * points[None, :] % period
    angles = phases.astype(jnp.float32) * (2.0 * math.pi / period)
    return (jnp.cos(angles), jnp.sin(angles))


def x_terms(cos_table, sin_table, values):
    stack_count, x_count, y_count = values.shape
    waves = cos_table.shape[0]
    table = jnp.concatenate([cos_table, -sin_table], axis=0)
    flat = jnp.transpose(values, (1, 0, 2)).reshape(x_count, stack_count * y_count)
    product = jnp.dot(
        table, flat, precision=lax.Precision.HIGHEST, preferred_element_type=jnp.float32
    )
    product = product.reshape(2, waves, stack_count, y_count)
    return jnp.transpose(product, (1, 0, 2, 3))


def y_terms(cos_table, sin_table, spectra):
    rows, parts, stack_count, y_count = spectra.shape
    waves = cos_table.shape[0]
    table = jnp.concatenate([cos_table, sin_table], axis=0)
    flat = spectra.reshape(rows * parts * stack_count, y_count)
    product = jnp.dot(
        flat, table.T, precision=lax.Precision.HIGHEST, preferred_element_type=jnp.float32
    )
    product = product.reshape(rows, parts, stack_count, 2, waves)
    real_part = product[:, 0, :, 0] + product[:, 1, :, 1]
    imag_part = product[:, 1, :, 0] - product[:, 0, :, 1]
    return jnp.stack([real_part, imag_part], axis=1)


def plain_shards(nx, ny, fields, wave_order, kept_mask):
    x_every = jnp.arange(nx, dtype=jnp.int32)
    x_cos, x_sin = wave_angles(wave_order, x_every, nx)
    partial_terms = x_terms(
        x_cos, x_sin, lax.all_to_all(fields, "gx", split_axis=2, concat_axis=1, tiled=True)
    )
    spectra = lax.all_to_all(partial_terms, "gx", split_axis=0, concat_axis=3, tiled=True)
    y_every = jnp.arange(ny, dtype=jnp.int32)
    y_cos, y_sin = wave_angles(y_every, y_every, ny)
    y_spectra = y_terms(
        y_cos, y_sin, lax.all_to_all(spectra, "gy", split_axis=0, concat_axis=3, tiled=True)
    )
    result = lax.all_to_all(y_spectra, "gy", split_axis=3, concat_axis=0, tiled=True)
    weight = kept_mask.astype(jnp.float32) * (1.0 / math.sqrt(nx * ny))
    return jnp.transpose(result, (1, 2, 0, 3)) * weight[None, None]


def fits(gx, gy, stack_count, nx, ny, kept):
    levels = stack_count // HALVES
    if gx != X_RADIX or gy != Y_RADIX or levels != gy or stack_count % HALVES:
        return False
    lanes = ny // gy // (gx // levels)
    return (
        lanes % LANES == 0
        and ny == Y_RADIX * Y_RADIX * LANES
        and nx % (X_RADIX * LANES) == 0
        and kept % (X_RADIX * LANES) == 0
        and kept <= nx
        and kept // (gx * gy) % (16 * PIECES) == 0
    )


def solution(mesh):
    gx, gy = mesh.shape["gx"], mesh.shape["gy"]

    def call(fields, wave_order, kept_mask):
        stack_count, nx, ny = fields.shape
        if fits(gx, gy, stack_count, nx, ny, wave_order.shape[0]):
            body = partial(fast_shards, gx, gy, nx, ny)
        else:
            body = partial(plain_shards, nx, ny)
        return jax.shard_map(
            body,
            mesh=mesh,
            in_specs=(P(None, "gx", "gy"), P(), P("gx", "gy")),
            out_specs=P(None, None, "gx", "gy"),
            check_vma=False,
        )(fields, wave_order, kept_mask)

    return call
```

```python
import math
from functools import partial

import jax
import jax.numpy as jnp
from jax import lax
from jax.experimental import pallas as pl
from jax.experimental.pallas import tpu as pltpu
from jax.sharding import PartitionSpec as P


X_RADIX = 8
Y_RADIX = 4
HALVES = 2
PIECES = 2
LANES = 128


def roots(numbers, period):
    angles = (numbers % period).astype(jnp.float32) * (2.0 * math.pi / period)
    return jnp.cos(angles), jnp.sin(angles)


def two_parts(values):
    high = lax.reduce_precision(values, 8, 7)
    return high.astype(jnp.bfloat16), (values - high).astype(jnp.bfloat16)


def x_table(period, kept, zero):
    points = jnp.arange(period // X_RADIX, dtype=jnp.int32) + zero
    units = jnp.arange(kept // X_RADIX, dtype=jnp.int32) * X_RADIX
    pairs = jnp.array([[0, 4], [1, 7], [2, 6], [3, 5]], dtype=jnp.int32)
    waves = pairs[:, :, None] + units[None, None, :]
    cos, sin = roots(waves[..., None] * points, period)
    table = jnp.stack([cos, sin], axis=2).reshape(4, 4 * units.shape[0], points.shape[0])
    return jnp.concatenate(two_parts(table), axis=2)


def y_table(period, scale, zero):
    short = period // Y_RADIX
    ids = jnp.arange(short, dtype=jnp.int32) + zero
    cos, sin = roots(ids[:, None] * ids[None, :], short)
    half = short // 2
    table = jnp.concatenate([cos[:, :half], sin[:, :half], cos[:, half:], sin[:, half:]], axis=1)
    return jnp.stack(two_parts(table * scale))


def y_twiddles(period, zero):
    ids = jnp.arange(period // Y_RADIX, dtype=jnp.int32) + zero
    cos, sin = roots(jnp.arange(Y_RADIX, dtype=jnp.int32)[:, None] * ids[None, :], period)
    return jnp.concatenate([cos, sin], axis=0)


IN_VMEM = pl.BlockSpec(memory_space=pltpu.VMEM)
IN_HBM = pl.BlockSpec(memory_space=pltpu.HBM)
LIMIT = pltpu.CompilerParams(vmem_limit_bytes=32 << 20)


def in_hbm(array):
    return pltpu.with_memory_space_constraint(array, pltpu.HBM)


def on_chip(*arrays):
    return [pltpu.with_memory_space_constraint(array, pltpu.VMEM) for array in arrays]


def dot(left, right):
    return jnp.dot(left, right, preferred_element_type=jnp.float32)


def split(values):
    high = values.astype(jnp.bfloat16)
    return high, (values - high.astype(jnp.float32)).astype(jnp.bfloat16)


def copy_all(pairs, semaphore):
    copies = [
        pltpu.make_async_copy(source, target, semaphore.at[at])
        for at, (source, target) in enumerate(pairs)
    ]
    for copy in copies:
        copy.start()
    return copies


def column_block(fields_ref, first, columns, to, lanes):
    if columns == 1:
        return fields_ref.at[first + to]
    start = pl.multiple_of(to % columns * lanes, LANES)
    return fields_ref.at[first + to // columns, :, pl.ds(start, lanes)]


def pack_body(first, columns, me_ref, fields_ref, *refs):
    outs, semaphore = refs[:-1], refs[-1]
    lanes = outs[0].shape[1]
    pairs = [
        (column_block(fields_ref, first, columns, jnp.bitwise_xor(me_ref[0], step), lanes), out)
        for step, out in enumerate(outs, 1)
    ]
    for copy in copy_all(pairs, semaphore):
        copy.wait()


def pack(me, fields, first, columns):
    stack_count, rows, width = fields.shape
    lanes = width // columns
    count = (stack_count // HALVES) * columns - 1
    return pl.pallas_call(
        partial(pack_body, first, columns),
        grid_spec=pltpu.PrefetchScalarGridSpec(
            num_scalar_prefetch=1,
            grid=(1,),
            in_specs=[IN_HBM],
            out_specs=[IN_VMEM] * count,
            scratch_shapes=[pltpu.SemaphoreType.DMA((count,))],
        ),
        out_shape=[pltpu.HBM((rows, lanes), jnp.float32)] * count,
        compiler_params=LIMIT,
        name="pack",
    )(me, in_hbm(fields))


def one_body(first, step, me_ref, fields_ref, out_ref, semaphore):
    place = first + jnp.bitwise_xor(me_ref[0], step)
    copy_all([(fields_ref.at[place], out_ref)], semaphore)[0].wait()


def pack_one(me, fields, first, step):
    return pl.pallas_call(
        partial(one_body, first, step),
        grid_spec=pltpu.PrefetchScalarGridSpec(
            num_scalar_prefetch=1,
            grid=(1,),
            in_specs=[IN_HBM],
            out_specs=IN_VMEM,
            scratch_shapes=[pltpu.SemaphoreType.DMA((1,))],
        ),
        out_shape=pltpu.VMEM(fields.shape[1:], jnp.float32),
        compiler_params=LIMIT,
        name="pack_one",
    )(me, in_hbm(fields))


def x_body(gy, first, columns, me_ref, where_ref, fields_ref, *refs):
    others, table_ref = refs[: X_RADIX - 1], refs[X_RADIX - 1]
    outs = refs[X_RADIX : X_RADIX + PIECES]
    line_ref, real_ref, imag_ref, semaphore = refs[X_RADIX + PIECES :]
    me = me_ref[0]
    points, lanes = line_ref.shape[1:]
    own = copy_all([(column_block(fields_ref, first, columns, me, lanes), line_ref.at[me])], semaphore)
    for step, ref in enumerate(others, 1):
        line_ref[jnp.bitwise_xor(me, step)] = ref[...]
    own[0].wait()
    units = real_ref.shape[0] // X_RADIX
    half = math.sqrt(0.5)
    f = [line_ref[at] for at in range(X_RADIX)]
    a = [f[at] + f[at + 4] for at in range(4)]
    d = [f[at] - f[at + 4] for at in range(4)]
    even, odd = a[0] + a[2], a[1] + a[3]
    less, more = (d[1] - d[3]) * half, (d[1] + d[3]) * half
    groups = (
        (0, 4, even + odd, even - odd),
        (1, 7, d[0] + less, -(d[2] + more)),
        (2, 6, a[0] - a[2], -(a[1] - a[3])),
        (3, 5, d[0] - less, d[2] - more),
    )
    for at, (c, e, left, right) in enumerate(groups):
        high, low = split(jnp.concatenate([left, right], axis=1))
        top = table_ref[at, :, :points]
        product = dot(top, high) + dot(table_ref[at, :, points:], high) + dot(top, low)
        cos_c, sin_c = product[:units], product[units : 2 * units]
        cos_e, sin_e = product[2 * units : 3 * units], product[3 * units :]
        rows_c, rows_e = pl.ds(c * units, units), pl.ds(e * units, units)
        if c == 0:
            real_ref[rows_c] = cos_c[:, :lanes]
            imag_ref[rows_c] = -sin_c[:, :lanes]
            real_ref[rows_e] = cos_e[:, lanes:]
            imag_ref[rows_e] = -sin_e[:, lanes:]
        else:
            real_ref[rows_c] = cos_c[:, :lanes] + sin_c[:, lanes:]
            imag_ref[rows_c] = cos_c[:, lanes:] - sin_c[:, :lanes]
            real_ref[rows_e] = cos_e[:, :lanes] - sin_e[:, lanes:]
            imag_ref[rows_e] = -cos_e[:, lanes:] - sin_e[:, :lanes]

    count, _, rows, _ = outs[0].shape

    def place(to, carry):
        start = to // gy * (gy * PIECES) + to % gy
        for piece, out_ref in enumerate(outs):
            for row in range(rows):
                source = where_ref[(start + piece * gy) * rows + row]
                out_ref[to, 0, pl.ds(row, 1), :] = real_ref[pl.ds(source, 1), :]
                out_ref[to, 1, pl.ds(row, 1), :] = imag_ref[pl.ds(source, 1), :]
        return carry

    lax.fori_loop(0, count, place, 0)


def x_lines(me, where, fields, first, columns, others, table, gx, gy):
    rows, lanes = others[0].shape
    kept = where.shape[0]
    out = (gx * gy, 2, kept // (gx * gy * PIECES), lanes)
    return pl.pallas_call(
        partial(x_body, gy, first, columns),
        grid_spec=pltpu.PrefetchScalarGridSpec(
            num_scalar_prefetch=2,
            grid=(1,),
            in_specs=[IN_HBM] + [IN_VMEM] * X_RADIX,
            out_specs=[IN_VMEM] * PIECES,
            scratch_shapes=[
                pltpu.VMEM((X_RADIX, rows, lanes), jnp.float32),
                pltpu.VMEM((kept, lanes), jnp.float32),
                pltpu.VMEM((kept, lanes), jnp.float32),
                pltpu.SemaphoreType.DMA((1,)),
            ],
        ),
        out_shape=[pltpu.HBM(out, jnp.float32)] * PIECES,
        compiler_params=LIMIT,
        name="x_lines",
    )(me, where, in_hbm(fields), *on_chip(*others, table))


def y_body(me_ref, in_ref, twiddle_ref, table_ref, *refs):
    outs = refs[:Y_RADIX]
    high_ref, low_ref, wave_ref = refs[Y_RADIX:]
    me = me_ref[0]
    sources, _, rows, lanes = in_ref.shape
    short = table_ref.shape[1]
    columns = short // lanes
    levels = sources // (Y_RADIX * columns)
    block = levels * rows
    for level in range(levels):
        for column in range(columns):
            base = (level * columns + column) * Y_RADIX
            re = [in_ref[base + at, 0] for at in range(Y_RADIX)]
            im = [in_ref[base + at, 1] for at in range(Y_RADIX)]
            even_r, even_i, odd_r, odd_i = re[0] + re[2], im[0] + im[2], re[1] + re[3], im[1] + im[3]
            less_r, less_i, more_r, more_i = re[0] - re[2], im[0] - im[2], re[1] - re[3], im[1] - im[3]
            folded = (
                (even_r + odd_r, even_i + odd_i),
                (less_r + more_i, less_i - more_r),
                (even_r - odd_r, even_i - odd_i),
                (less_r - more_i, less_i + more_r),
            )
            span = pl.ds(column * lanes, lanes)
            for c, (real, imag) in enumerate(folded):
                if c:
                    cos = twiddle_ref[pl.ds(c, 1), span]
                    sin = twiddle_ref[pl.ds(Y_RADIX + c, 1), span]
                    real, imag = real * cos + imag * sin, imag * cos - real * sin
                for part, values in enumerate((real, imag)):
                    high, low = split(values)
                    at = pl.ds((c * 2 + part) * block + level * rows, rows)
                    high_ref[at, span] = high
                    low_ref[at, span] = low
    whole = dot(high_ref[...], table_ref[0]) + dot(low_ref[...], table_ref[0]) + dot(high_ref[...], table_ref[1])
    for c in range(Y_RADIX):
        product = whole[c * 2 * block : (c + 1) * 2 * block]
        for to in range(Y_RADIX):
            start = (to // 2 * Y_RADIX + to % 2) * LANES
            by_cos, by_sin = slice(start, start + LANES), slice(start + 2 * LANES, start + 3 * LANES)
            wave_ref[c, to, :block] = product[:block, by_cos] + product[block:, by_sin]
            wave_ref[c, to, block:] = product[block:, by_cos] - product[:block, by_sin]
    lane = lax.broadcasted_iota(jnp.int32, (rows, LANES), 1)
    residue = lane % Y_RADIX
    for step in range(Y_RADIX):
        to = jnp.bitwise_xor(me, step)
        for part in range(2):
            for level in range(levels):
                at = pl.ds(part * block + level * rows, rows)
                pieces = [wave_ref[c, to, at, :] for c in range(Y_RADIX)]
                for tile in range(Y_RADIX):
                    index = tile * (LANES // Y_RADIX) + lane // Y_RADIX
                    value = jnp.take_along_axis(pieces[0], index, axis=1, mode="promise_in_bounds")
                    for c in range(1, Y_RADIX):
                        other = jnp.take_along_axis(pieces[c], index, axis=1, mode="promise_in_bounds")
                        value = jnp.where(residue == c, other, value)
                    outs[step][part, level, :, pl.ds(tile * LANES, LANES)] = value


def y_lines(me, spectra, twiddles, table):
    sources, _, rows, lanes = spectra.shape
    short = table.shape[1]
    levels = sources * lanes // (Y_RADIX * short)
    out = (2, levels, rows, short)
    tall = Y_RADIX * 2 * levels * rows
    return pl.pallas_call(
        y_body,
        grid_spec=pltpu.PrefetchScalarGridSpec(
            num_scalar_prefetch=1,
            grid=(1,),
            in_specs=[IN_VMEM] * 3,
            out_specs=[IN_VMEM] * Y_RADIX,
            scratch_shapes=[
                pltpu.VMEM((tall, short), jnp.bfloat16),
                pltpu.VMEM((tall, short), jnp.bfloat16),
                pltpu.VMEM((Y_RADIX, Y_RADIX, 2 * levels * rows, short // Y_RADIX), jnp.float32),
            ],
        ),
        out_shape=[pltpu.HBM(out, jnp.float32)] * Y_RADIX,
        compiler_params=LIMIT,
        name="y_lines",
    )(me, in_hbm(spectra), twiddles, table)


def finish_body(piece, me_ref, *refs):
    blocks, mask_ref, out_ref = refs[:Y_RADIX], refs[Y_RADIX], refs[-3]
    out_buffer, out_semaphore = refs[-2:]
    _, levels, rows, _ = blocks[0].shape
    rows_out = rows * Y_RADIX
    leaving = []
    for level in range(levels):
        for step in range(Y_RADIX):
            at = pl.ds(pl.multiple_of(jnp.bitwise_xor(me_ref[0], step) * rows, rows), rows)
            masked = pl.multiple_of(piece * rows_out + jnp.bitwise_xor(me_ref[0], step) * rows, rows)
            weight = mask_ref[pl.ds(masked, rows), :].astype(jnp.float32)
            for part in range(2):
                out_buffer[level, part, at, :] = blocks[step][part, level] * weight
        target = out_ref.at[:, level, pl.ds(piece * rows_out, rows_out), :]
        leaving += copy_all([(out_buffer.at[level], target)], out_semaphore.at[level])
    for copy in leaving:
        copy.wait()


def finish(me, blocks, kept_mask, piece, stack_count, before):
    _, levels, rows, width = blocks[0].shape
    rows_out = rows * Y_RADIX
    extra = [] if before is None else [before]
    return pl.pallas_call(
        partial(finish_body, piece),
        grid_spec=pltpu.PrefetchScalarGridSpec(
            num_scalar_prefetch=1,
            grid=(1,),
            in_specs=[IN_VMEM] * Y_RADIX
            + [IN_VMEM]
            + [IN_HBM] * len(extra),
            out_specs=IN_HBM,
            scratch_shapes=[
                pltpu.VMEM((levels, 2, rows_out, width), jnp.float32),
                pltpu.SemaphoreType.DMA((levels, 1)),
            ],
        ),
        out_shape=jax.ShapeDtypeStruct((2, stack_count) + kept_mask.shape, jnp.float32),
        input_output_aliases={} if before is None else {2 + Y_RADIX: 0},
        compiler_params=LIMIT,
        name="finish",
    )(me, *on_chip(*blocks, kept_mask), *extra)


def turn(values):
    lane = lax.broadcasted_iota(jnp.int32, values.shape, 1)
    rolled = pltpu.roll(values, LANES // 2, 1)
    return jnp.where(lane < LANES // 2, rolled, -rolled)


def y_first_body(scale, first, me_ref, fields_ref, *refs):
    others = refs[: Y_RADIX - 1]
    twiddle_ref, table_ref = refs[Y_RADIX - 1 : Y_RADIX + 1]
    outs = refs[Y_RADIX + 1 : Y_RADIX + 1 + X_RADIX]
    field_ref, wave_ref, semaphore = refs[Y_RADIX + 1 + X_RADIX :]
    me_x, me_y = me_ref[0], me_ref[1]
    _, rows, short = field_ref.shape
    half = short // 2
    own = copy_all([(column_block(fields_ref, first, 1, me_y, short), field_ref.at[me_y])], semaphore)
    for step, ref in enumerate(others, 1):
        field_ref[jnp.bitwise_xor(me_y, step)] = ref[...]
    own[0].wait()
    even, odd = field_ref[0] + field_ref[2], field_ref[1] + field_ref[3]
    less, more = field_ref[0] - field_ref[2], field_ref[1] - field_ref[3]
    folded = ((even + odd, None), (less, -more), (even - odd, None), (less, more))
    for c, (real, imag) in enumerate(folded):
        if c:
            cos, sin = twiddle_ref[pl.ds(c, 1), :], twiddle_ref[pl.ds(Y_RADIX + c, 1), :]
            if imag is None:
                real, imag = real * cos, -real * sin
            else:
                real, imag = real * cos + imag * sin, imag * cos - real * sin
        tall = real if imag is None else jnp.concatenate([real, imag], axis=0)
        high, low = split(tall)
        top, bottom = table_ref[0, :, :short], table_ref[1, :, :short]
        product = dot(high, top) + dot(low, top) + dot(high, bottom)
        by_cos, by_sin = product[:, :half], product[:, half:]
        if imag is None:
            point = lax.broadcasted_iota(jnp.int32, real.shape, 1)
            top = jnp.sum(jnp.where(point % 2 == 0, real, -real), axis=1, keepdims=True) * scale
            unit = lax.broadcasted_iota(jnp.int32, by_sin.shape, 1)
            wave_ref[c] = by_cos
            wave_ref[Y_RADIX + c] = jnp.where(unit == 0, top, -by_sin)
        else:
            wave_ref[c] = by_cos[:rows] + by_sin[rows:]
            wave_ref[Y_RADIX + c] = by_cos[rows:] - by_sin[:rows]
    chunk, group = 32, LANES // X_RADIX

    def place(at, carry):
        span = pl.ds(pl.multiple_of(at * chunk, chunk), chunk)
        lane = lax.broadcasted_iota(jnp.int32, (chunk, LANES), 1)
        for side in range(2):
            units = pl.ds(side * LANES, LANES)
            tiles = [wave_ref[number, span, units] for number in range(X_RADIX)]
            for bit in (1, 2, 4):
                upper = lane // (group * bit) % 2 == 1
                for low in range(X_RADIX):
                    if low & bit:
                        continue
                    one, two = tiles[low], tiles[low + bit]
                    tiles[low] = jnp.where(upper, pltpu.roll(two, group * bit, 1), one)
                    tiles[low + bit] = jnp.where(upper, two, pltpu.roll(one, LANES - group * bit, 1))
            for number, tile in enumerate(tiles):
                wave_ref[number, span, units] = tile
        return carry

    lax.fori_loop(0, rows // chunk, place, 0)
    for step, out in enumerate(outs):
        out[...] = wave_ref[jnp.bitwise_xor(me_x, step)]


def y_first(me, scale, fields, first, others, twiddles, table):
    rows, short = others[0].shape
    out = (rows, 2 * LANES)
    return pl.pallas_call(
        partial(y_first_body, scale, first),
        grid_spec=pltpu.PrefetchScalarGridSpec(
            num_scalar_prefetch=1,
            grid=(1,),
            in_specs=[IN_HBM] + [IN_VMEM] * (Y_RADIX + 1),
            out_specs=[IN_VMEM] * X_RADIX,
            scratch_shapes=[
                pltpu.VMEM((Y_RADIX, rows, short), jnp.float32),
                pltpu.VMEM((X_RADIX, rows, 2 * LANES), jnp.float32),
                pltpu.SemaphoreType.DMA((1,)),
            ],
        ),
        out_shape=[pltpu.HBM(out, jnp.float32)] * X_RADIX,
        compiler_params=LIMIT,
        name="y_first",
    )(me, in_hbm(fields), *on_chip(*others), twiddles, table)


def x_second_body(me_ref, where_ref, *refs):
    blocks = refs[:X_RADIX]
    table_ref, out_ref, fold_ref, wave_ref = refs[X_RADIX:]
    me = me_ref[0]
    points = blocks[0].shape[0]
    units = wave_ref.shape[1] // X_RADIX
    for step, ref in enumerate(blocks):
        fold_ref[jnp.bitwise_xor(me, step)] = ref[...]
    half = math.sqrt(0.5)
    for side in range(2):
        span = pl.ds(side * LANES, LANES)
        f = [fold_ref[at, :, span] for at in range(X_RADIX)]
        a = [f[at] + f[at + 4] for at in range(4)]
        d = [f[at] - f[at + 4] for at in range(4)]
        even, odd, less, more = a[0] + a[2], a[1] + a[3], a[0] - a[2], turn(a[1] - a[3])
        across, along = turn(d[2]), turn(d[1] + d[3])
        one = (d[1] - d[3] + along) * half
        three = (along - d[1] + d[3]) * half
        folded = {
            0: even + odd,
            4: even - odd,
            2: less + more,
            6: less - more,
            1: d[0] + across + one,
            5: d[0] + across - one,
            3: d[0] - across + three,
            7: d[0] - across - three,
        }
        for c, values in folded.items():
            fold_ref[c, :, span] = values
    lane = lax.broadcasted_iota(jnp.int32, (points, 2 * LANES), 1)
    sign = jnp.where(lane % LANES < LANES // 2, 1.0, -1.0)
    lane = lax.broadcasted_iota(jnp.int32, (units, LANES), 1)
    special = jnp.logical_and(lane % (LANES // 2) == 0, me == 0)
    for at, pair in enumerate(((0, 4), (1, 7), (2, 6), (3, 5))):
        for side, c in enumerate(pair):
            data = jnp.concatenate([fold_ref[c], fold_ref[-c % X_RADIX] * sign], axis=1)
            high, low = split(data)
            rows = pl.ds(side * 2 * units, 2 * units)
            top = table_ref[at, rows, :points]
            product = dot(top, high) + dot(table_ref[at, rows, points:], high) + dot(top, low)
            plus_low, plus_high, minus_low, minus_high = (
                product[:units, piece * LANES : (piece + 1) * LANES]
                + turn(product[units:, piece * LANES : (piece + 1) * LANES])
                for piece in range(4)
            )
            rows = pl.ds(c * units, units)
            wave_ref[0, rows] = jnp.where(special, (plus_low + minus_low) * 0.5, plus_low)
            wave_ref[1, rows] = plus_high
            wave_ref[2, rows] = jnp.where(special, turn(plus_low - minus_low) * 0.5, minus_high)
            wave_ref[3, rows] = jnp.where(special, minus_high, minus_low)

    count, rows, _ = out_ref.shape
    unroll = 32

    def place(at, carry):
        to, start = at // (rows // unroll) * Y_RADIX, at % (rows // unroll) * unroll
        for row in range(unroll):
            source = where_ref[at * unroll + row]
            for piece in range(Y_RADIX):
                out_ref[to + piece, pl.ds(start + row, 1), :] = wave_ref[piece, pl.ds(source, 1), :]
        return carry

    lax.fori_loop(0, count // Y_RADIX * (rows // unroll), place, 0)


def x_second(me, where, blocks, table, gx):
    points, lanes = blocks[0].shape
    kept = where.shape[0]
    out = (gx * Y_RADIX, kept // gx, LANES)
    return pl.pallas_call(
        x_second_body,
        grid_spec=pltpu.PrefetchScalarGridSpec(
            num_scalar_prefetch=2,
            grid=(1,),
            in_specs=[IN_VMEM] * (X_RADIX + 1),
            out_specs=IN_VMEM,
            scratch_shapes=[
                pltpu.VMEM((X_RADIX, points, lanes), jnp.float32),
                pltpu.VMEM((Y_RADIX, kept, LANES), jnp.float32),
            ],
        ),
        out_shape=pltpu.HBM(out, jnp.float32),
        compiler_params=LIMIT,
        name="x_second",
    )(me, where, in_hbm(blocks[0]), *on_chip(*blocks[1:]), table)


def finish_second_body(first, me_ref, blocks_ref, mask_ref, before_ref, out_ref, *refs):
    out_buffer, out_semaphore = refs
    mirrored = me_ref[0] >= Y_RADIX // 2
    _, levels, rows, _ = blocks_ref.shape
    chunk, group = 32, LANES // X_RADIX

    def place(level, at):
        span = pl.ds(pl.multiple_of(at * chunk, chunk), chunk)
        lane = lax.broadcasted_iota(jnp.int32, (chunk, LANES), 1)
        left = lane < LANES // 2
        wanted = jnp.where(mirrored, (LANES - lane) % LANES, lane)
        local = wanted % (LANES // 2)
        index = wanted - local + local % Y_RADIX * group + local // Y_RADIX
        for tile in range(Y_RADIX):
            body = jnp.where(mirrored, Y_RADIX - 1 - tile, tile)
            head = jnp.where(mirrored, (Y_RADIX - tile) % Y_RADIX, tile)
            here, there = blocks_ref[2 * body, level, span, :], blocks_ref[2 * body + 1, level, span, :]
            start = blocks_ref[2 * head, level, span, :]
            real = jnp.where(left, here, pltpu.roll(there, LANES // 2, 1))
            imag = jnp.where(left, pltpu.roll(here, LANES // 2, 1), there)
            lanes = pl.ds(tile * LANES, LANES)
            weight = mask_ref[span, lanes].astype(jnp.float32)
            for part, (values, edge) in enumerate(((real, start), (imag, pltpu.roll(start, LANES // 2, 1)))):
                values = jnp.take_along_axis(values, index, axis=1, mode="promise_in_bounds")
                out_buffer[level, part, span, lanes] = jnp.where(lane == 0, edge, values) * weight

    leaving = []
    for level in range(levels):

        def step(at, carry):
            place(level, at)
            return carry

        lax.fori_loop(0, rows // chunk, step, 0)
        leaving += copy_all([(out_buffer.at[level], out_ref.at[:, first + level])], out_semaphore.at[level])
    for copy in leaving:
        copy.wait()


def finish_second(me, blocks, kept_mask, first, before):
    _, levels, _, _ = blocks.shape
    return pl.pallas_call(
        partial(finish_second_body, first),
        grid_spec=pltpu.PrefetchScalarGridSpec(
            num_scalar_prefetch=1,
            grid=(1,),
            in_specs=[IN_VMEM, IN_VMEM, IN_HBM],
            out_specs=IN_HBM,
            scratch_shapes=[
                pltpu.VMEM((levels, 2) + kept_mask.shape, jnp.float32),
                pltpu.SemaphoreType.DMA((levels, 1)),
            ],
        ),
        out_shape=jax.ShapeDtypeStruct(before.shape, jnp.float32),
        input_output_aliases={3: 0},
        compiler_params=LIMIT,
        name="finish_second",
    )(me, *on_chip(blocks), kept_mask, before)


def exchange(blocks, axis, size):
    arrived = {}
    for step in sorted(range(1, size), key=lambda step: (step < size // 2, step)):
        pairs = [(at, at ^ step) for at in range(size)]
        arrived[step] = lax.ppermute(blocks[step - 1], axis, pairs)
    return [arrived[step] for step in range(1, size)]


def fast_shards(gx, gy, nx, ny, fields, wave_order, kept_mask):
    stack_count = fields.shape[0]
    kept = wave_order.shape[0]
    levels = stack_count // HALVES
    columns = gx // levels
    me_x, me_y = lax.axis_index("gx"), lax.axis_index("gy")
    zero = me_x // gx
    x_me, y_me = me_x.reshape(1).astype(jnp.int32), me_y.reshape(1).astype(jnp.int32)
    where = (wave_order % X_RADIX) * (kept // X_RADIX) + wave_order // X_RADIX
    both_me = jnp.concatenate([x_me, y_me])
    scale = 1.0 / math.sqrt(nx * ny)
    whole = ("gx", "gy")
    second = levels
    leaving = []
    for step in range(1, gy):
        if step == gy // 2:
            leaving.append(pack_one(y_me, fields, second, step))
            continue
        place = second + jnp.bitwise_xor(me_y, step)
        leaving.append(lax.dynamic_index_in_dim(fields, place, 0, keepdims=False))
    fields_second = exchange(leaving, "gy", gy)
    lines = exchange(pack(x_me, fields, 0, columns), "gx", gx)
    tables = x_table(nx, kept, zero), y_table(ny, scale, zero), y_twiddles(ny, zero)
    table_x, table_y, twiddles = lax.optimization_barrier(tables)
    spectra = x_lines(x_me, where, fields, 0, columns, lines, table_x, gx, gy)
    spectra = list(spectra)
    for piece in range(PIECES):
        spectra[piece] = lax.all_to_all(spectra[piece], whole, split_axis=0, concat_axis=0, tiled=True)
    half_waves = y_first(both_me, scale, fields, second, fields_second, twiddles, table_y)
    half_waves = [half_waves[0]] + exchange(half_waves[1:], "gx", gx)
    owned = x_second(x_me, where, half_waves, table_x, gx)
    owned = lax.all_to_all(owned, whole, split_axis=0, concat_axis=0, tiled=True)
    result = None
    for piece in range(PIECES):
        waves = y_lines(y_me, spectra[piece], twiddles, table_y)
        waves = [waves[0]] + exchange(waves[1:], "gy", gy)
        if piece == PIECES - 1:
            owned = owned.reshape((gx, gy) + owned.shape[1:])
            result = finish_second(y_me, owned, kept_mask, second, result)
        result = finish(y_me, waves, kept_mask, piece, stack_count, result)
    return result


def wave_angles(wave_ids, points, period):
    phases = wave_ids[:, None] * points[None, :] % period
    angles = phases.astype(jnp.float32) * (2.0 * math.pi / period)
    return (jnp.cos(angles), jnp.sin(angles))


def x_terms(cos_table, sin_table, values):
    stack_count, x_count, y_count = values.shape
    waves = cos_table.shape[0]
    table = jnp.concatenate([cos_table, -sin_table], axis=0)
    flat = jnp.transpose(values, (1, 0, 2)).reshape(x_count, stack_count * y_count)
    product = jnp.dot(
        table, flat, precision=lax.Precision.HIGHEST, preferred_element_type=jnp.float32
    )
    product = product.reshape(2, waves, stack_count, y_count)
    return jnp.transpose(product, (1, 0, 2, 3))


def y_terms(cos_table, sin_table, spectra):
    rows, parts, stack_count, y_count = spectra.shape
    waves = cos_table.shape[0]
    table = jnp.concatenate([cos_table, sin_table], axis=0)
    flat = spectra.reshape(rows * parts * stack_count, y_count)
    product = jnp.dot(
        flat, table.T, precision=lax.Precision.HIGHEST, preferred_element_type=jnp.float32
    )
    product = product.reshape(rows, parts, stack_count, 2, waves)
    real_part = product[:, 0, :, 0] + product[:, 1, :, 1]
    imag_part = product[:, 1, :, 0] - product[:, 0, :, 1]
    return jnp.stack([real_part, imag_part], axis=1)


def plain_shards(nx, ny, fields, wave_order, kept_mask):
    x_every = jnp.arange(nx, dtype=jnp.int32)
    x_cos, x_sin = wave_angles(wave_order, x_every, nx)
    partial_terms = x_terms(
        x_cos, x_sin, lax.all_to_all(fields, "gx", split_axis=2, concat_axis=1, tiled=True)
    )
    spectra = lax.all_to_all(partial_terms, "gx", split_axis=0, concat_axis=3, tiled=True)
    y_every = jnp.arange(ny, dtype=jnp.int32)
    y_cos, y_sin = wave_angles(y_every, y_every, ny)
    y_spectra = y_terms(
        y_cos, y_sin, lax.all_to_all(spectra, "gy", split_axis=0, concat_axis=3, tiled=True)
    )
    result = lax.all_to_all(y_spectra, "gy", split_axis=3, concat_axis=0, tiled=True)
    weight = kept_mask.astype(jnp.float32) * (1.0 / math.sqrt(nx * ny))
    return jnp.transpose(result, (1, 2, 0, 3)) * weight[None, None]


def fits(gx, gy, stack_count, nx, ny, kept):
    levels = stack_count // HALVES
    if gx != X_RADIX or gy != Y_RADIX or levels != gy or stack_count % HALVES:
        return False
    lanes = ny // gy // (gx // levels)
    return (
        lanes % LANES == 0
        and ny == Y_RADIX * Y_RADIX * LANES
        and nx % (X_RADIX * LANES) == 0
        and kept % (X_RADIX * LANES) == 0
        and kept <= nx
        and kept // (gx * gy) % (16 * PIECES) == 0
    )


def solution(mesh):
    gx, gy = mesh.shape["gx"], mesh.shape["gy"]

    def call(fields, wave_order, kept_mask):
        stack_count, nx, ny = fields.shape
        if fits(gx, gy, stack_count, nx, ny, wave_order.shape[0]):
            body = partial(fast_shards, gx, gy, nx, ny)
        else:
            body = partial(plain_shards, nx, ny)
        return jax.shard_map(
            body,
            mesh=mesh,
            in_specs=(P(None, "gx", "gy"), P(), P("gx", "gy")),
            out_specs=P(None, None, "gx", "gy"),
            check_vma=False,
        )(fields, wave_order, kept_mask)

    return call
```

```python
import math
from functools import partial

import jax
import jax.numpy as jnp
from jax import lax
from jax.experimental import pallas as pl
from jax.experimental.pallas import tpu as pltpu
from jax.sharding import PartitionSpec as P


X_RADIX = 8
Y_RADIX = 4
HALVES = 2
PIECES = 2
LANES = 128


def roots(numbers, period):
    angles = (numbers % period).astype(jnp.float32) * (2.0 * math.pi / period)
    return jnp.cos(angles), jnp.sin(angles)


def two_parts(values):
    high = lax.reduce_precision(values, 8, 7)
    return high.astype(jnp.bfloat16), (values - high).astype(jnp.bfloat16)


def x_table(period, kept, zero):
    points = jnp.arange(period // X_RADIX, dtype=jnp.int32) + zero
    units = jnp.arange(kept // X_RADIX, dtype=jnp.int32) * X_RADIX
    pairs = jnp.array([[0, 4], [1, 7], [2, 6], [3, 5]], dtype=jnp.int32)
    waves = pairs[:, :, None] + units[None, None, :]
    cos, sin = roots(waves[..., None] * points, period)
    table = jnp.stack([cos, sin], axis=2).reshape(4, 4 * units.shape[0], points.shape[0])
    return jnp.concatenate(two_parts(table), axis=2)


def y_table(period, scale, zero):
    short = period // Y_RADIX
    ids = jnp.arange(short, dtype=jnp.int32) + zero
    cos, sin = roots(ids[:, None] * ids[None, :], short)
    half = short // 2
    table = jnp.concatenate([cos[:, :half], sin[:, :half], cos[:, half:], sin[:, half:]], axis=1)
    return jnp.stack(two_parts(table * scale))


def y_twiddles(period, zero):
    ids = jnp.arange(period // Y_RADIX, dtype=jnp.int32) + zero
    cos, sin = roots(jnp.arange(Y_RADIX, dtype=jnp.int32)[:, None] * ids[None, :], period)
    return jnp.concatenate([cos, sin], axis=0)


IN_VMEM = pl.BlockSpec(memory_space=pltpu.VMEM)
IN_HBM = pl.BlockSpec(memory_space=pltpu.HBM)
LIMIT = pltpu.CompilerParams(vmem_limit_bytes=32 << 20)


def in_hbm(array):
    return pltpu.with_memory_space_constraint(array, pltpu.HBM)


def on_chip(*arrays):
    return [pltpu.with_memory_space_constraint(array, pltpu.VMEM) for array in arrays]


def dot(left, right):
    return jnp.dot(left, right, preferred_element_type=jnp.float32)


def split(values):
    high = values.astype(jnp.bfloat16)
    return high, (values - high.astype(jnp.float32)).astype(jnp.bfloat16)


def copy_all(pairs, semaphore):
    copies = [
        pltpu.make_async_copy(source, target, semaphore.at[at])
        for at, (source, target) in enumerate(pairs)
    ]
    for copy in copies:
        copy.start()
    return copies


def column_block(fields_ref, first, columns, to, lanes):
    if columns == 1:
        return fields_ref.at[first + to]
    start = pl.multiple_of(to % columns * lanes, LANES)
    return fields_ref.at[first + to // columns, :, pl.ds(start, lanes)]


def pack_body(first, columns, me_ref, fields_ref, *refs):
    outs, semaphore = refs[:-1], refs[-1]
    lanes = outs[0].shape[1]
    pairs = [
        (column_block(fields_ref, first, columns, jnp.bitwise_xor(me_ref[0], step), lanes), out)
        for step, out in enumerate(outs, 1)
    ]
    for copy in copy_all(pairs, semaphore):
        copy.wait()


def pack(me, fields, first, columns):
    stack_count, rows, width = fields.shape
    lanes = width // columns
    count = (stack_count // HALVES) * columns - 1
    return pl.pallas_call(
        partial(pack_body, first, columns),
        grid_spec=pltpu.PrefetchScalarGridSpec(
            num_scalar_prefetch=1,
            grid=(1,),
            in_specs=[IN_HBM],
            out_specs=[IN_VMEM] * count,
            scratch_shapes=[pltpu.SemaphoreType.DMA((count,))],
        ),
        out_shape=[
            (pltpu.VMEM if step > count // 2 else pltpu.HBM)((rows, lanes), jnp.float32)
            for step in range(1, count + 1)
        ],
        compiler_params=LIMIT,
        name="pack",
    )(me, in_hbm(fields))


def one_body(first, step, me_ref, fields_ref, out_ref, semaphore):
    place = first + jnp.bitwise_xor(me_ref[0], step)
    copy_all([(fields_ref.at[place], out_ref)], semaphore)[0].wait()


def pack_one(me, fields, first, step):
    return pl.pallas_call(
        partial(one_body, first, step),
        grid_spec=pltpu.PrefetchScalarGridSpec(
            num_scalar_prefetch=1,
            grid=(1,),
            in_specs=[IN_HBM],
            out_specs=IN_VMEM,
            scratch_shapes=[pltpu.SemaphoreType.DMA((1,))],
        ),
        out_shape=pltpu.VMEM(fields.shape[1:], jnp.float32),
        compiler_params=LIMIT,
        name="pack_one",
    )(me, in_hbm(fields))


def x_body(gy, first, columns, me_ref, where_ref, fields_ref, *refs):
    others, table_ref = refs[: X_RADIX - 1], refs[X_RADIX - 1]
    outs = refs[X_RADIX : X_RADIX + PIECES]
    line_ref, real_ref, imag_ref, semaphore = refs[X_RADIX + PIECES :]
    me = me_ref[0]
    points, lanes = line_ref.shape[1:]
    own = copy_all([(column_block(fields_ref, first, columns, me, lanes), line_ref.at[me])], semaphore)
    for step, ref in enumerate(others, 1):
        line_ref[jnp.bitwise_xor(me, step)] = ref[...]
    own[0].wait()
    units = real_ref.shape[0] // X_RADIX
    half = math.sqrt(0.5)
    f = [line_ref[at] for at in range(X_RADIX)]
    a = [f[at] + f[at + 4] for at in range(4)]
    d = [f[at] - f[at + 4] for at in range(4)]
    even, odd = a[0] + a[2], a[1] + a[3]
    less, more = (d[1] - d[3]) * half, (d[1] + d[3]) * half
    groups = (
        (0, 4, even + odd, even - odd),
        (1, 7, d[0] + less, -(d[2] + more)),
        (2, 6, a[0] - a[2], -(a[1] - a[3])),
        (3, 5, d[0] - less, d[2] - more),
    )
    for at, (c, e, left, right) in enumerate(groups):
        high, low = split(jnp.concatenate([left, right], axis=1))
        top = table_ref[at, :, :points]
        product = dot(top, high) + dot(table_ref[at, :, points:], high) + dot(top, low)
        cos_c, sin_c = product[:units], product[units : 2 * units]
        cos_e, sin_e = product[2 * units : 3 * units], product[3 * units :]
        rows_c, rows_e = pl.ds(c * units, units), pl.ds(e * units, units)
        if c == 0:
            real_ref[rows_c] = cos_c[:, :lanes]
            imag_ref[rows_c] = -sin_c[:, :lanes]
            real_ref[rows_e] = cos_e[:, lanes:]
            imag_ref[rows_e] = -sin_e[:, lanes:]
        else:
            real_ref[rows_c] = cos_c[:, :lanes] + sin_c[:, lanes:]
            imag_ref[rows_c] = cos_c[:, lanes:] - sin_c[:, :lanes]
            real_ref[rows_e] = cos_e[:, :lanes] - sin_e[:, lanes:]
            imag_ref[rows_e] = -cos_e[:, lanes:] - sin_e[:, :lanes]

    count, _, rows, _ = outs[0].shape

    def place(to, carry):
        start = to // gy * (gy * PIECES) + to % gy
        for piece, out_ref in enumerate(outs):
            for row in range(rows):
                source = where_ref[(start + piece * gy) * rows + row]
                out_ref[to, 0, pl.ds(row, 1), :] = real_ref[pl.ds(source, 1), :]
                out_ref[to, 1, pl.ds(row, 1), :] = imag_ref[pl.ds(source, 1), :]
        return carry

    lax.fori_loop(0, count, place, 0)


def x_lines(me, where, fields, first, columns, others, table, gx, gy):
    rows, lanes = others[0].shape
    kept = where.shape[0]
    out = (gx * gy, 2, kept // (gx * gy * PIECES), lanes)
    return pl.pallas_call(
        partial(x_body, gy, first, columns),
        grid_spec=pltpu.PrefetchScalarGridSpec(
            num_scalar_prefetch=2,
            grid=(1,),
            in_specs=[IN_HBM] + [IN_VMEM] * X_RADIX,
            out_specs=[IN_VMEM] * PIECES,
            scratch_shapes=[
                pltpu.VMEM((X_RADIX, rows, lanes), jnp.float32),
                pltpu.VMEM((kept, lanes), jnp.float32),
                pltpu.VMEM((kept, lanes), jnp.float32),
                pltpu.SemaphoreType.DMA((1,)),
            ],
        ),
        out_shape=[pltpu.HBM(out, jnp.float32)] * PIECES,
        compiler_params=LIMIT,
        name="x_lines",
    )(me, where, in_hbm(fields), *on_chip(*others, table))


def y_body(me_ref, in_ref, twiddle_ref, table_ref, *refs):
    outs = refs[:Y_RADIX]
    high_ref, low_ref, wave_ref = refs[Y_RADIX:]
    me = me_ref[0]
    sources, _, rows, lanes = in_ref.shape
    short = table_ref.shape[1]
    columns = short // lanes
    levels = sources // (Y_RADIX * columns)
    block = levels * rows
    for level in range(levels):
        for column in range(columns):
            base = (level * columns + column) * Y_RADIX
            re = [in_ref[base + at, 0] for at in range(Y_RADIX)]
            im = [in_ref[base + at, 1] for at in range(Y_RADIX)]
            even_r, even_i, odd_r, odd_i = re[0] + re[2], im[0] + im[2], re[1] + re[3], im[1] + im[3]
            less_r, less_i, more_r, more_i = re[0] - re[2], im[0] - im[2], re[1] - re[3], im[1] - im[3]
            folded = (
                (even_r + odd_r, even_i + odd_i),
                (less_r + more_i, less_i - more_r),
                (even_r - odd_r, even_i - odd_i),
                (less_r - more_i, less_i + more_r),
            )
            span = pl.ds(column * lanes, lanes)
            for c, (real, imag) in enumerate(folded):
                if c:
                    cos = twiddle_ref[pl.ds(c, 1), span]
                    sin = twiddle_ref[pl.ds(Y_RADIX + c, 1), span]
                    real, imag = real * cos + imag * sin, imag * cos - real * sin
                for part, values in enumerate((real, imag)):
                    high, low = split(values)
                    at = pl.ds((c * 2 + part) * block + level * rows, rows)
                    high_ref[at, span] = high
                    low_ref[at, span] = low
    whole = dot(high_ref[...], table_ref[0]) + dot(low_ref[...], table_ref[0]) + dot(high_ref[...], table_ref[1])
    for c in range(Y_RADIX):
        product = whole[c * 2 * block : (c + 1) * 2 * block]
        for to in range(Y_RADIX):
            start = (to // 2 * Y_RADIX + to % 2) * LANES
            by_cos, by_sin = slice(start, start + LANES), slice(start + 2 * LANES, start + 3 * LANES)
            wave_ref[c, to, :block] = product[:block, by_cos] + product[block:, by_sin]
            wave_ref[c, to, block:] = product[block:, by_cos] - product[:block, by_sin]
    lane = lax.broadcasted_iota(jnp.int32, (rows, LANES), 1)
    residue = lane % Y_RADIX
    for step in range(Y_RADIX):
        to = jnp.bitwise_xor(me, step)
        for part in range(2):
            for level in range(levels):
                at = pl.ds(part * block + level * rows, rows)
                pieces = [wave_ref[c, to, at, :] for c in range(Y_RADIX)]
                for tile in range(Y_RADIX):
                    index = tile * (LANES // Y_RADIX) + lane // Y_RADIX
                    value = jnp.take_along_axis(pieces[0], index, axis=1, mode="promise_in_bounds")
                    for c in range(1, Y_RADIX):
                        other = jnp.take_along_axis(pieces[c], index, axis=1, mode="promise_in_bounds")
                        value = jnp.where(residue == c, other, value)
                    outs[step][part, level, :, pl.ds(tile * LANES, LANES)] = value


def y_lines(me, spectra, twiddles, table):
    sources, _, rows, lanes = spectra.shape
    short = table.shape[1]
    levels = sources * lanes // (Y_RADIX * short)
    out = (2, levels, rows, short)
    tall = Y_RADIX * 2 * levels * rows
    return pl.pallas_call(
        y_body,
        grid_spec=pltpu.PrefetchScalarGridSpec(
            num_scalar_prefetch=1,
            grid=(1,),
            in_specs=[IN_VMEM] * 3,
            out_specs=[IN_VMEM] * Y_RADIX,
            scratch_shapes=[
                pltpu.VMEM((tall, short), jnp.bfloat16),
                pltpu.VMEM((tall, short), jnp.bfloat16),
                pltpu.VMEM((Y_RADIX, Y_RADIX, 2 * levels * rows, short // Y_RADIX), jnp.float32),
            ],
        ),
        out_shape=[pltpu.HBM(out, jnp.float32)] + [pltpu.VMEM(out, jnp.float32)] * (Y_RADIX - 1),
        compiler_params=LIMIT,
        name="y_lines",
    )(me, in_hbm(spectra), twiddles, table)


def finish_body(piece, me_ref, *refs):
    blocks, mask_ref, out_ref = refs[:Y_RADIX], refs[Y_RADIX], refs[-3]
    out_buffer, out_semaphore = refs[-2:]
    _, levels, rows, _ = blocks[0].shape
    rows_out = rows * Y_RADIX
    leaving = []
    for level in range(levels):
        for step in range(Y_RADIX):
            at = pl.ds(pl.multiple_of(jnp.bitwise_xor(me_ref[0], step) * rows, rows), rows)
            masked = pl.multiple_of(piece * rows_out + jnp.bitwise_xor(me_ref[0], step) * rows, rows)
            weight = mask_ref[pl.ds(masked, rows), :].astype(jnp.float32)
            for part in range(2):
                out_buffer[level, part, at, :] = blocks[step][part, level] * weight
        target = out_ref.at[:, level, pl.ds(piece * rows_out, rows_out), :]
        leaving += copy_all([(out_buffer.at[level], target)], out_semaphore.at[level])
    for copy in leaving:
        copy.wait()


def finish(me, blocks, kept_mask, piece, stack_count, before):
    _, levels, rows, width = blocks[0].shape
    rows_out = rows * Y_RADIX
    extra = [] if before is None else [before]
    return pl.pallas_call(
        partial(finish_body, piece),
        grid_spec=pltpu.PrefetchScalarGridSpec(
            num_scalar_prefetch=1,
            grid=(1,),
            in_specs=[IN_VMEM] * Y_RADIX
            + [IN_VMEM]
            + [IN_HBM] * len(extra),
            out_specs=IN_HBM,
            scratch_shapes=[
                pltpu.VMEM((levels, 2, rows_out, width), jnp.float32),
                pltpu.SemaphoreType.DMA((levels, 1)),
            ],
        ),
        out_shape=jax.ShapeDtypeStruct((2, stack_count) + kept_mask.shape, jnp.float32),
        input_output_aliases={} if before is None else {2 + Y_RADIX: 0},
        compiler_params=LIMIT,
        name="finish",
    )(me, *on_chip(*blocks, kept_mask), *extra)


def turn(values):
    lane = lax.broadcasted_iota(jnp.int32, values.shape, 1)
    rolled = pltpu.roll(values, LANES // 2, 1)
    return jnp.where(lane < LANES // 2, rolled, -rolled)


def y_first_body(scale, first, me_ref, fields_ref, *refs):
    others = refs[: Y_RADIX - 1]
    twiddle_ref, table_ref = refs[Y_RADIX - 1 : Y_RADIX + 1]
    outs = refs[Y_RADIX + 1 : Y_RADIX + 1 + X_RADIX]
    field_ref, wave_ref, semaphore = refs[Y_RADIX + 1 + X_RADIX :]
    me_x, me_y = me_ref[0], me_ref[1]
    _, rows, short = field_ref.shape
    half = short // 2
    own = copy_all([(column_block(fields_ref, first, 1, me_y, short), field_ref.at[me_y])], semaphore)
    for step, ref in enumerate(others, 1):
        field_ref[jnp.bitwise_xor(me_y, step)] = ref[...]
    own[0].wait()
    even, odd = field_ref[0] + field_ref[2], field_ref[1] + field_ref[3]
    less, more = field_ref[0] - field_ref[2], field_ref[1] - field_ref[3]
    folded = ((even + odd, None), (less, -more), (even - odd, None), (less, more))
    for c, (real, imag) in enumerate(folded):
        if c:
            cos, sin = twiddle_ref[pl.ds(c, 1), :], twiddle_ref[pl.ds(Y_RADIX + c, 1), :]
            if imag is None:
                real, imag = real * cos, -real * sin
            else:
                real, imag = real * cos + imag * sin, imag * cos - real * sin
        tall = real if imag is None else jnp.concatenate([real, imag], axis=0)
        high, low = split(tall)
        top, bottom = table_ref[0, :, :short], table_ref[1, :, :short]
        product = dot(high, top) + dot(low, top) + dot(high, bottom)
        by_cos, by_sin = product[:, :half], product[:, half:]
        if imag is None:
            point = lax.broadcasted_iota(jnp.int32, real.shape, 1)
            top = jnp.sum(jnp.where(point % 2 == 0, real, -real), axis=1, keepdims=True) * scale
            unit = lax.broadcasted_iota(jnp.int32, by_sin.shape, 1)
            wave_ref[c] = by_cos
            wave_ref[Y_RADIX + c] = jnp.where(unit == 0, top, -by_sin)
        else:
            wave_ref[c] = by_cos[:rows] + by_sin[rows:]
            wave_ref[Y_RADIX + c] = by_cos[rows:] - by_sin[:rows]
    chunk, group = 32, LANES // X_RADIX

    def place(at, carry):
        span = pl.ds(pl.multiple_of(at * chunk, chunk), chunk)
        lane = lax.broadcasted_iota(jnp.int32, (chunk, LANES), 1)
        for side in range(2):
            units = pl.ds(side * LANES, LANES)
            tiles = [wave_ref[number, span, units] for number in range(X_RADIX)]
            for bit in (1, 2, 4):
                upper = lane // (group * bit) % 2 == 1
                for low in range(X_RADIX):
                    if low & bit:
                        continue
                    one, two = tiles[low], tiles[low + bit]
                    tiles[low] = jnp.where(upper, pltpu.roll(two, group * bit, 1), one)
                    tiles[low + bit] = jnp.where(upper, two, pltpu.roll(one, LANES - group * bit, 1))
            for number, tile in enumerate(tiles):
                wave_ref[number, span, units] = tile
        return carry

    lax.fori_loop(0, rows // chunk, place, 0)
    for step, out in enumerate(outs):
        out[...] = wave_ref[jnp.bitwise_xor(me_x, step)]


def y_first(me, scale, fields, first, others, twiddles, table):
    rows, short = others[0].shape
    out = (rows, 2 * LANES)
    return pl.pallas_call(
        partial(y_first_body, scale, first),
        grid_spec=pltpu.PrefetchScalarGridSpec(
            num_scalar_prefetch=1,
            grid=(1,),
            in_specs=[IN_HBM] + [IN_VMEM] * (Y_RADIX + 1),
            out_specs=[IN_VMEM] * X_RADIX,
            scratch_shapes=[
                pltpu.VMEM((Y_RADIX, rows, short), jnp.float32),
                pltpu.VMEM((X_RADIX, rows, 2 * LANES), jnp.float32),
                pltpu.SemaphoreType.DMA((1,)),
            ],
        ),
        out_shape=[pltpu.HBM(out, jnp.float32)] * X_RADIX,
        compiler_params=LIMIT,
        name="y_first",
    )(me, in_hbm(fields), *on_chip(*others), twiddles, table)


def x_second_body(me_ref, where_ref, *refs):
    blocks = refs[:X_RADIX]
    table_ref, out_ref, fold_ref, wave_ref = refs[X_RADIX:]
    me = me_ref[0]
    points = blocks[0].shape[0]
    units = wave_ref.shape[1] // X_RADIX
    for step, ref in enumerate(blocks):
        fold_ref[jnp.bitwise_xor(me, step)] = ref[...]
    half = math.sqrt(0.5)
    for side in range(2):
        span = pl.ds(side * LANES, LANES)
        f = [fold_ref[at, :, span] for at in range(X_RADIX)]
        a = [f[at] + f[at + 4] for at in range(4)]
        d = [f[at] - f[at + 4] for at in range(4)]
        even, odd, less, more = a[0] + a[2], a[1] + a[3], a[0] - a[2], turn(a[1] - a[3])
        across, along = turn(d[2]), turn(d[1] + d[3])
        one = (d[1] - d[3] + along) * half
        three = (along - d[1] + d[3]) * half
        folded = {
            0: even + odd,
            4: even - odd,
            2: less + more,
            6: less - more,
            1: d[0] + across + one,
            5: d[0] + across - one,
            3: d[0] - across + three,
            7: d[0] - across - three,
        }
        for c, values in folded.items():
            fold_ref[c, :, span] = values
    lane = lax.broadcasted_iota(jnp.int32, (points, 2 * LANES), 1)
    sign = jnp.where(lane % LANES < LANES // 2, 1.0, -1.0)
    lane = lax.broadcasted_iota(jnp.int32, (units, LANES), 1)
    special = jnp.logical_and(lane % (LANES // 2) == 0, me == 0)
    for at, pair in enumerate(((0, 4), (1, 7), (2, 6), (3, 5))):
        for side, c in enumerate(pair):
            data = jnp.concatenate([fold_ref[c], fold_ref[-c % X_RADIX] * sign], axis=1)
            high, low = split(data)
            rows = pl.ds(side * 2 * units, 2 * units)
            top = table_ref[at, rows, :points]
            product = dot(top, high) + dot(table_ref[at, rows, points:], high) + dot(top, low)
            plus_low, plus_high, minus_low, minus_high = (
                product[:units, piece * LANES : (piece + 1) * LANES]
                + turn(product[units:, piece * LANES : (piece + 1) * LANES])
                for piece in range(4)
            )
            rows = pl.ds(c * units, units)
            wave_ref[0, rows] = jnp.where(special, (plus_low + minus_low) * 0.5, plus_low)
            wave_ref[1, rows] = plus_high
            wave_ref[2, rows] = jnp.where(special, turn(plus_low - minus_low) * 0.5, minus_high)
            wave_ref[3, rows] = jnp.where(special, minus_high, minus_low)

    count, rows, _ = out_ref.shape
    unroll = 32

    def place(at, carry):
        to, start = at // (rows // unroll) * Y_RADIX, at % (rows // unroll) * unroll
        for row in range(unroll):
            source = where_ref[at * unroll + row]
            for piece in range(Y_RADIX):
                out_ref[to + piece, pl.ds(start + row, 1), :] = wave_ref[piece, pl.ds(source, 1), :]
        return carry

    lax.fori_loop(0, count // Y_RADIX * (rows // unroll), place, 0)


def x_second(me, where, blocks, table, gx):
    points, lanes = blocks[0].shape
    kept = where.shape[0]
    out = (gx * Y_RADIX, kept // gx, LANES)
    return pl.pallas_call(
        x_second_body,
        grid_spec=pltpu.PrefetchScalarGridSpec(
            num_scalar_prefetch=2,
            grid=(1,),
            in_specs=[IN_VMEM] * (X_RADIX + 1),
            out_specs=IN_VMEM,
            scratch_shapes=[
                pltpu.VMEM((X_RADIX, points, lanes), jnp.float32),
                pltpu.VMEM((Y_RADIX, kept, LANES), jnp.float32),
            ],
        ),
        out_shape=pltpu.HBM(out, jnp.float32),
        compiler_params=LIMIT,
        name="x_second",
    )(me, where, in_hbm(blocks[0]), *on_chip(*blocks[1:]), table)


def finish_second_body(first, me_ref, blocks_ref, mask_ref, before_ref, out_ref, *refs):
    out_buffer, out_semaphore = refs
    mirrored = me_ref[0] >= Y_RADIX // 2
    _, levels, rows, _ = blocks_ref.shape
    chunk, group = 32, LANES // X_RADIX

    def place(level, at):
        span = pl.ds(pl.multiple_of(at * chunk, chunk), chunk)
        lane = lax.broadcasted_iota(jnp.int32, (chunk, LANES), 1)
        left = lane < LANES // 2
        wanted = jnp.where(mirrored, (LANES - lane) % LANES, lane)
        local = wanted % (LANES // 2)
        index = wanted - local + local % Y_RADIX * group + local // Y_RADIX
        for tile in range(Y_RADIX):
            body = jnp.where(mirrored, Y_RADIX - 1 - tile, tile)
            head = jnp.where(mirrored, (Y_RADIX - tile) % Y_RADIX, tile)
            here, there = blocks_ref[2 * body, level, span, :], blocks_ref[2 * body + 1, level, span, :]
            start = blocks_ref[2 * head, level, span, :]
            real = jnp.where(left, here, pltpu.roll(there, LANES // 2, 1))
            imag = jnp.where(left, pltpu.roll(here, LANES // 2, 1), there)
            lanes = pl.ds(tile * LANES, LANES)
            weight = mask_ref[span, lanes].astype(jnp.float32)
            for part, (values, edge) in enumerate(((real, start), (imag, pltpu.roll(start, LANES // 2, 1)))):
                values = jnp.take_along_axis(values, index, axis=1, mode="promise_in_bounds")
                out_buffer[level, part, span, lanes] = jnp.where(lane == 0, edge, values) * weight

    leaving = []
    for level in range(levels):

        def step(at, carry):
            place(level, at)
            return carry

        lax.fori_loop(0, rows // chunk, step, 0)
        leaving += copy_all([(out_buffer.at[level], out_ref.at[:, first + level])], out_semaphore.at[level])
    for copy in leaving:
        copy.wait()


def finish_second(me, blocks, kept_mask, first, before):
    _, levels, _, _ = blocks.shape
    return pl.pallas_call(
        partial(finish_second_body, first),
        grid_spec=pltpu.PrefetchScalarGridSpec(
            num_scalar_prefetch=1,
            grid=(1,),
            in_specs=[IN_VMEM, IN_VMEM, IN_HBM],
            out_specs=IN_HBM,
            scratch_shapes=[
                pltpu.VMEM((levels, 2) + kept_mask.shape, jnp.float32),
                pltpu.SemaphoreType.DMA((levels, 1)),
            ],
        ),
        out_shape=jax.ShapeDtypeStruct(before.shape, jnp.float32),
        input_output_aliases={3: 0},
        compiler_params=LIMIT,
        name="finish_second",
    )(me, *on_chip(blocks), kept_mask, before)


def exchange(blocks, axis, size):
    arrived = {}
    for step in sorted(range(1, size), key=lambda step: (step < size // 2, step)):
        pairs = [(at, at ^ step) for at in range(size)]
        arrived[step] = lax.ppermute(blocks[step - 1], axis, pairs)
    return [arrived[step] for step in range(1, size)]


def fast_shards(gx, gy, nx, ny, fields, wave_order, kept_mask):
    stack_count = fields.shape[0]
    kept = wave_order.shape[0]
    levels = stack_count // HALVES
    columns = gx // levels
    me_x, me_y = lax.axis_index("gx"), lax.axis_index("gy")
    zero = me_x // gx
    x_me, y_me = me_x.reshape(1).astype(jnp.int32), me_y.reshape(1).astype(jnp.int32)
    where = (wave_order % X_RADIX) * (kept // X_RADIX) + wave_order // X_RADIX
    both_me = jnp.concatenate([x_me, y_me])
    scale = 1.0 / math.sqrt(nx * ny)
    whole = ("gx", "gy")
    second = levels
    leaving = []
    for step in range(1, gy):
        if step == gy // 2:
            leaving.append(pack_one(y_me, fields, second, step))
            continue
        place = second + jnp.bitwise_xor(me_y, step)
        leaving.append(lax.dynamic_index_in_dim(fields, place, 0, keepdims=False))
    fields_second = exchange(leaving, "gy", gy)
    lines = exchange(pack(x_me, fields, 0, columns), "gx", gx)
    tables = x_table(nx, kept, zero), y_table(ny, scale, zero), y_twiddles(ny, zero)
    table_x, table_y, twiddles = lax.optimization_barrier(tables)
    spectra = x_lines(x_me, where, fields, 0, columns, lines, table_x, gx, gy)
    spectra = list(spectra)
    for piece in range(PIECES):
        spectra[piece] = lax.all_to_all(spectra[piece], whole, split_axis=0, concat_axis=0, tiled=True)
    half_waves = y_first(both_me, scale, fields, second, fields_second, twiddles, table_y)
    half_waves = [half_waves[0]] + exchange(half_waves[1:], "gx", gx)
    owned = x_second(x_me, where, half_waves, table_x, gx)
    owned = lax.all_to_all(owned, whole, split_axis=0, concat_axis=0, tiled=True)
    result = None
    for piece in range(PIECES):
        waves = y_lines(y_me, spectra[piece], twiddles, table_y)
        waves = [waves[0]] + exchange(waves[1:], "gy", gy)
        if piece == PIECES - 1:
            owned = owned.reshape((gx, gy) + owned.shape[1:])
            result = finish_second(y_me, owned, kept_mask, second, result)
        result = finish(y_me, waves, kept_mask, piece, stack_count, result)
    return result


def wave_angles(wave_ids, points, period):
    phases = wave_ids[:, None] * points[None, :] % period
    angles = phases.astype(jnp.float32) * (2.0 * math.pi / period)
    return (jnp.cos(angles), jnp.sin(angles))


def x_terms(cos_table, sin_table, values):
    stack_count, x_count, y_count = values.shape
    waves = cos_table.shape[0]
    table = jnp.concatenate([cos_table, -sin_table], axis=0)
    flat = jnp.transpose(values, (1, 0, 2)).reshape(x_count, stack_count * y_count)
    product = jnp.dot(
        table, flat, precision=lax.Precision.HIGHEST, preferred_element_type=jnp.float32
    )
    product = product.reshape(2, waves, stack_count, y_count)
    return jnp.transpose(product, (1, 0, 2, 3))


def y_terms(cos_table, sin_table, spectra):
    rows, parts, stack_count, y_count = spectra.shape
    waves = cos_table.shape[0]
    table = jnp.concatenate([cos_table, sin_table], axis=0)
    flat = spectra.reshape(rows * parts * stack_count, y_count)
    product = jnp.dot(
        flat, table.T, precision=lax.Precision.HIGHEST, preferred_element_type=jnp.float32
    )
    product = product.reshape(rows, parts, stack_count, 2, waves)
    real_part = product[:, 0, :, 0] + product[:, 1, :, 1]
    imag_part = product[:, 1, :, 0] - product[:, 0, :, 1]
    return jnp.stack([real_part, imag_part], axis=1)


def plain_shards(nx, ny, fields, wave_order, kept_mask):
    x_every = jnp.arange(nx, dtype=jnp.int32)
    x_cos, x_sin = wave_angles(wave_order, x_every, nx)
    partial_terms = x_terms(
        x_cos, x_sin, lax.all_to_all(fields, "gx", split_axis=2, concat_axis=1, tiled=True)
    )
    spectra = lax.all_to_all(partial_terms, "gx", split_axis=0, concat_axis=3, tiled=True)
    y_every = jnp.arange(ny, dtype=jnp.int32)
    y_cos, y_sin = wave_angles(y_every, y_every, ny)
    y_spectra = y_terms(
        y_cos, y_sin, lax.all_to_all(spectra, "gy", split_axis=0, concat_axis=3, tiled=True)
    )
    result = lax.all_to_all(y_spectra, "gy", split_axis=3, concat_axis=0, tiled=True)
    weight = kept_mask.astype(jnp.float32) * (1.0 / math.sqrt(nx * ny))
    return jnp.transpose(result, (1, 2, 0, 3)) * weight[None, None]


def fits(gx, gy, stack_count, nx, ny, kept):
    levels = stack_count // HALVES
    if gx != X_RADIX or gy != Y_RADIX or levels != gy or stack_count % HALVES:
        return False
    lanes = ny // gy // (gx // levels)
    return (
        lanes % LANES == 0
        and ny == Y_RADIX * Y_RADIX * LANES
        and nx % (X_RADIX * LANES) == 0
        and kept % (X_RADIX * LANES) == 0
        and kept <= nx
        and kept // (gx * gy) % (16 * PIECES) == 0
    )


def solution(mesh):
    gx, gy = mesh.shape["gx"], mesh.shape["gy"]

    def call(fields, wave_order, kept_mask):
        stack_count, nx, ny = fields.shape
        if fits(gx, gy, stack_count, nx, ny, wave_order.shape[0]):
            body = partial(fast_shards, gx, gy, nx, ny)
        else:
            body = partial(plain_shards, nx, ny)
        return jax.shard_map(
            body,
            mesh=mesh,
            in_specs=(P(None, "gx", "gy"), P(), P("gx", "gy")),
            out_specs=P(None, None, "gx", "gy"),
            check_vma=False,
        )(fields, wave_order, kept_mask)

    return call
```
